128 devices in a mesh: team: 8 (over x, core), inner: 16 (over z, y).
Axes of the slice: x: 4, y: 4, z: 4, core: 2. Of those that a mesh axis runs over, the one named last changes fastest.
Arguments:
- queries: float32 [16384, 1024], P(('team', 'inner')), may hold values from -8 to 8
- passages: float32 [16384, 1024], P(('team', 'inner')), may hold values from -8 to 8
- positive: int32 [16384], P(('team', 'inner')), may hold values from 0 to 16383, as said below
Outputs:
- grad_queries: float32 [16384, 1024], P(('team', 'inner'))
- grad_passages: float32 [16384, 1024], P(('team', 'inner'))
The draws below stay inside these ranges and needn't reach their ends.
Inputs may be any that keep to these rules, and one draw needn't show every extreme that they name: `positive`: a permutation of the passage indices 0 to 16383.
All inputs are finite; a program needn't handle non-finite values.
Results may differ from the reference program's by a relative error of at most 0.014.
Values may be sent and summed in bfloat16 or wider, within the bound.
A program may use at most 64 MiB of HBM per device.

```python
import jax
import jax.numpy as jnp
from jax import lax

D = 1024
ROWS_DEV = 128
B = 16384
N_TEAM = 8
N_INNER = 16


cluster_members = 512


subspace_rank = 16


def latent_rows(key):
    keys = jax.random.split(jax.random.fold_in(key, 11), 11)
    cluster_count = max(2, B // cluster_members)
    centers = jax.random.truncated_normal(keys[0], -4.0, 4.0, (cluster_count, D), jnp.float32)
    member = jax.random.randint(keys[1], (B,), 0, cluster_count)
    target_order = jax.random.permutation(keys[2], B).astype(jnp.int32)
    basis = jax.random.truncated_normal(keys[8], -4.0, 4.0, (subspace_rank, D), jnp.float32)
    passage_mix = jax.random.truncated_normal(keys[9], -4.0, 4.0, (B, subspace_rank), jnp.float32)
    query_mix = jax.random.truncated_normal(keys[10], -4.0, 4.0, (B, subspace_rank), jnp.float32)
    passage_sub = jnp.dot(passage_mix, basis, precision=lax.Precision.HIGHEST) / jnp.sqrt(jnp.float32(subspace_rank))
    query_sub = jnp.dot(query_mix, basis, precision=lax.Precision.HIGHEST) / jnp.sqrt(jnp.float32(subspace_rank))
    noise_rows = jax.random.truncated_normal(keys[3], -4.0, 4.0, (B, D), jnp.float32)
    passage_shape = 0.6 * centers[member] + 0.6 * passage_sub + 0.5 * noise_rows
    query_noise = jax.random.truncated_normal(keys[5], -4.0, 4.0, (B, D), jnp.float32)
    lowest = 0.1
    query_shape = 0.45 * passage_shape[target_order] + 0.6 * query_sub + 0.7 * query_noise
    passage_scale = jnp.exp(jax.random.uniform(keys[6], (B, 1), jnp.float32, jnp.log(lowest), 0.0))
    query_scale = jnp.exp(jax.random.uniform(keys[7], (B, 1), jnp.float32, jnp.log(lowest), 0.0))
    passage_values = jnp.clip(passage_scale * passage_shape, -8.0, 8.0)
    query_values = jnp.clip(query_scale * query_shape, -8.0, 8.0)
    return (target_order, passage_values, query_values)


def draw_positive(key, part):
    return latent_rows(key)[0]


def draw_passages(key, part):
    return latent_rows(key)[1].astype(jnp.float32)


def draw_queries(key, part):
    return latent_rows(key)[2].astype(jnp.float32)


def setup_inputs(seed: int = 0) -> dict:
    splits = jax.random.split(jax.random.key(seed), 4)
    return {
        "queries": draw_queries(jax.random.fold_in(splits[3], 71), 0),
        "passages": draw_passages(jax.random.fold_in(splits[3], 71), 0),
        "positive": draw_positive(jax.random.fold_in(splits[3], 71), 0),
    }


logit_scale_factor = 20.0
epsilon = 1e-06

def unit_rows(vectors):
    length = jnp.sqrt(lax.optimization_barrier(jnp.sum(vectors * vectors, axis=1, keepdims=True)) + epsilon)
    return (vectors / length, length)

def finish(unit_vectors, length, grad_raw):
    projection = lax.optimization_barrier(jnp.sum(unit_vectors * grad_raw, axis=1, keepdims=True))
    return (grad_raw - unit_vectors * projection) / length

def exponent(query_tile_rows, column_block):
    similarity_scores = lax.dot_general(query_tile_rows, column_block, (((1,), (1,)), ((), ())), preferred_element_type=jnp.float32)
    return jnp.exp(logit_scale_factor * similarity_scores)

def weights(query_tile_rows, column_block, target_block, row_block, column_block_total, first_column):
    exponentials = exponent(query_tile_rows, column_block)
    column_ids = first_column + lax.iota(jnp.int32, column_block.shape[0])
    is_target = (target_block[:, None] == column_ids[None, :]).astype(jnp.float32)
    combined = exponentials / row_block[:, None] + exponentials / column_block_total[None, :] - 2.0 * is_target
    return combined.astype(jnp.bfloat16)

def rounded_scores(values):
    narrow = lax.optimization_barrier(values.astype(jnp.bfloat16))
    return narrow.astype(jnp.float32)

def reference(queries, passages, positive):
    total_rows = queries.shape[0]
    query_unit, query_length = unit_rows(queries)
    passage_unit, passage_length = unit_rows(passages)
    query_round = query_unit.astype(jnp.bfloat16)
    passage_round = passage_unit.astype(jnp.bfloat16)
    block_rows = min(512, total_rows)
    block_count = total_rows // block_rows
    query_blocks = query_round.reshape(block_count, block_rows, D)

    def column_sums(running, query_tile_rows):
        exponentials = exponent(query_tile_rows, passage_round)
        return (running + lax.optimization_barrier(jnp.sum(exponentials, axis=0)), lax.optimization_barrier(jnp.sum(exponentials, axis=1)))
    column_total, row_blocks = lax.scan(column_sums, jnp.zeros((total_rows,), jnp.float32), query_blocks)
    row_total = row_blocks.reshape(total_rows)
    group_rows = total_rows // N_TEAM
    slot_columns = N_TEAM * ROWS_DEV
    group_queries = query_round.reshape(N_TEAM, group_rows, D)
    group_targets = positive.reshape(N_TEAM, group_rows)
    group_totals = row_total.reshape(N_TEAM, group_rows)
    slot_passages = passage_round.reshape(N_TEAM, N_INNER, ROWS_DEV, D).transpose(1, 0, 2, 3).reshape(N_INNER, slot_columns, D)

    def group_step(running, pieces):
        query_tile_rows, target_block, row_block = pieces
        loss_weight = weights(query_tile_rows, passage_round, target_block, row_block, column_total, 0)
        slot_weight = loss_weight.reshape(group_rows, N_TEAM, N_INNER, ROWS_DEV).transpose(2, 0, 1, 3).reshape(N_INNER, group_rows, slot_columns)

        def slot_part(pair):
            slot_weight_matrix, slot_probability = pair
            return rounded_scores(logit_scale_factor * jnp.dot(slot_weight_matrix, slot_probability, preferred_element_type=jnp.float32))
        parts = lax.map(slot_part, (slot_weight, slot_passages))
        query_contribution = lax.optimization_barrier(jnp.sum(parts, axis=0))
        passage_contribution = rounded_scores(logit_scale_factor * lax.dot_general(loss_weight, query_tile_rows, (((0,), (0,)), ((), ())), preferred_element_type=jnp.float32))
        return (running + passage_contribution, query_contribution)
    passage_grad, query_parts = lax.scan(group_step, jnp.zeros((total_rows, D), jnp.float32), (group_queries, group_targets, group_totals))
    grad_queries = finish(query_unit, query_length, query_parts.reshape(total_rows, D))
    grad_passages = finish(passage_unit, passage_length, passage_grad)
    return (grad_queries, grad_passages)
```

```python
import math

import jax
import jax.numpy as jnp
from jax import lax
from jax.experimental import pallas as pl
from jax.experimental.pallas import tpu as pltpu
from jax.sharding import PartitionSpec as P

MESH = pl.DeviceIdType.MESH
F32 = jnp.float32
BF16 = jnp.bfloat16

SCALE = 20.0
EXP2_SCALE = SCALE * math.log2(math.e)
EPSILON = 1e-06
RING = 4
ROWS = 128
HALF = 64
D = 1024
NQ = 2048
NP = 1024

PLACE = {
    (0, 0): 0, (0, 1): 1, (3, 0): 2, (1, 0): 3,
    (3, 1): 4, (1, 1): 5, (2, 0): 6, (2, 1): 7,
}
ORDER = sorted(PLACE, key=PLACE.get)
A, B = 0, 1
COPIES = 160


class Links:
    def __init__(self, send_sem, recv_sem):
        self.send_sem, self.recv_sem, self.copies = send_sem, recv_sem, {}

    def send(self, name, src, dst, device):
        i = len(self.copies)
        assert i < COPIES and name not in self.copies
        copy = pltpu.make_async_remote_copy(
            src_ref=src,
            dst_ref=dst,
            send_sem=self.send_sem.at[i],
            recv_sem=self.recv_sem.at[i],
            device_id=device,
            device_id_type=MESH,
        )
        copy.start()
        self.copies[name] = copy

    def arrived(self, name):
        self.copies[name].wait_recv()

    def drain(self):
        for copy in self.copies.values():
            copy.wait_send()


def kernel(
    q_hbm, p_hbm, pos_in, gq_hbm, gp_hbm,
    qf, pf, q_len, p_len, qbuf, pbuf, pos_buf, e_ref, w_ref, racc, cacc,
    row_tx, row_rx, col_tx, col_rx, row_tot, col_tot, qpart, ppart, q_d2d, q_rx, p_rx,
    local_sem, send_sem, recv_sem,
):
    team, inner = lax.axis_index("team"), lax.axis_index("inner")
    x, c = team // 2, team % 2
    z, y = inner // RING, inner % RING
    bit = y % 2

    def device(x, y, z, c):
        return {"team": x * 2 + c, "inner": z * RING + y}

    def q_device(r, s, t):
        yy = y if s == 0 else y + 1 - 2 * bit
        return device((x + r) % RING, yy, z, c if t == 0 else 1 - c)

    def p_device(r, s):
        return device(x, y if s == 0 else 3 - y, (z + r) % RING, c)

    q_peers = [(r, s, t) for r in range(RING) for s in range(2) for t in range(2)][1:]
    p_peers = [(r, s) for r in range(RING) for s in range(2)][1:]

    loads = [
        pltpu.make_async_copy(q_hbm, qf, local_sem.at[0]),
        pltpu.make_async_copy(p_hbm, pf, local_sem.at[1]),
    ]
    for load in loads:
        load.start()
    barrier = pltpu.get_barrier_semaphore()
    for peer in q_peers:
        pl.semaphore_signal(barrier, inc=1, device_id=q_device(*peer), device_id_type=MESH)
    for peer in p_peers:
        pl.semaphore_signal(barrier, inc=1, device_id=p_device(*peer), device_id_type=MESH)

    links = Links(send_sem, recv_sem)
    send, arrived = links.send, links.arrived

    def normalize(full, length_ref, rounded):
        v = full[...]
        length = jnp.sqrt(jnp.sum(v * v, axis=1, keepdims=True) + EPSILON)
        unit = v / length
        full[...] = unit
        length_ref[...] = jnp.broadcast_to(length, (ROWS, 128))
        rounded[pl.ds(0, ROWS), :] = unit.astype(BF16)

    loads[0].wait()
    normalize(qf, q_len, qbuf)
    loads[1].wait()
    normalize(pf, p_len, pbuf)
    pos_buf[0] = jnp.broadcast_to(pos_in[...], (8, 128))
    racc[...] = jnp.zeros_like(racc)
    cacc[...] = jnp.zeros_like(cacc)
    pl.semaphore_wait(barrier, len(q_peers) + len(p_peers))

    def q_at(place, half, t=0):
        return qbuf.at[pl.ds(PLACE[place] * 256 + t * ROWS + half * HALF, HALF), :]

    def p_at(place, half):
        return pbuf.at[pl.ds(PLACE[place] * ROWS + half * HALF, HALF), :]

    class Gather:
        def __init__(self, tag, at, right, left, pair, on_arrival):
            self.tag, self.at, self.on_arrival = tag, at, on_arrival
            self.to = {"x": right, "l": left, "y": pair}
            self.landed = {}

        def send(self, name, src, dst, half):
            self.landed[name] = (dst, half)
            send(self.tag + name, self.at(src, half), self.at(dst, half), self.to[name[0]])

        def take(self, name):
            arrived(self.tag + name)
            self.on_arrival(name, *self.landed[name])

        def begin(self):
            self.send("xA", (0, 0), (3, 0), A)
            self.send("lA", (0, 0), (1, 0), A)
            self.send("yB", (0, 0), (0, 1), B)
            self.send("xB", (0, 0), (3, 0), B)
            self.send("lB", (0, 0), (1, 0), B)
            self.send("yA", (0, 0), (0, 1), A)

        def first(self):
            self.take("xA")
            self.send("xA2", (3, 0), (2, 0), A)
            self.send("yA3", (3, 0), (3, 1), A)
            self.take("lA")
            self.send("yA1", (1, 0), (1, 1), A)
            self.take("yB")
            self.send("xPB", (0, 1), (3, 1), B)
            self.send("lPB", (0, 1), (1, 1), B)

        def second(self):
            self.take("xB")
            self.send("xB2", (3, 0), (2, 0), B)
            self.take("lB")
            self.take("yA")

        def third(self):
            self.take("lPB")
            self.send("lPB2", (1, 1), (2, 1), B)
            self.take("xA2")
            self.send("yA2", (2, 0), (2, 1), A)
            self.take("yA3")

        def fourth(self):
            self.take("xPB")
            self.take("yA1")

        def fifth(self):
            self.take("xB2")
            self.take("lPB2")
            self.take("yA2")

    sibling = q_device(0, 0, 1)

    def share(name, place, half):
        send("c" + name, q_at(place, half, 0), q_at(place, half, 1), sibling)

    qg = Gather("q", q_at, q_device(1, 0, 0), q_device(3, 0, 0), q_device(0, 1, 0), share)
    pg = Gather("p", p_at, p_device(1, 0), p_device(3, 0), p_device(0, 1), lambda *_: None)
    qg.begin()
    pg.begin()
    send("c", qbuf.at[pl.ds(0, ROWS), :], qbuf.at[pl.ds(ROWS, ROWS), :], sibling)
    for r, s, t in q_peers:
        slot = PLACE[(-r % RING, s)] * 2 + t
        send(f"pos{r}{s}{t}", pos_buf.at[0], pos_buf.at[slot], q_device(r, s, t))

    def scores(rows0, rows1, cols0, cols1):
        step, width = 512, 256

        @pl.loop(0, (rows1 - rows0) // step)
        def _(i):
            rows = pl.ds(pl.multiple_of(rows0 + i * step, step), step)
            for j in range(cols0, cols1, width):
                cols = pl.ds(j, width)
                s = lax.dot_general(
                    qbuf[rows, :],
                    pbuf[cols, :],
                    (((1,), (1,)), ((), ())),
                    preferred_element_type=F32,
                )
                e = jnp.exp2(s * EXP2_SCALE)
                e_ref[rows, cols] = e
                part = e[:, 0:128]
                for k in range(128, width, 128):
                    part = part + e[:, k : k + 128]
                racc[rows, :] += part
                cacc[:, cols] += jnp.sum(e.reshape(step // 8, 8, width), axis=0)

    for g in (qg, pg):
        g.first()
    for g in (qg, pg):
        g.second()
    arrived("c")
    for name in ("xA", "lA", "yB", "xB", "lB", "yA"):
        arrived("c" + name)
    scores(0, 1024, 0, 512)
    for g in (qg, pg):
        g.third()
    for g in (qg, pg):
        g.fourth()
    for name in ("lPB", "yA3", "xPB", "yA1"):
        arrived("c" + name)
    scores(0, 1024, 512, 768)
    scores(1024, 1536, 0, 768)
    for g in (qg, pg):
        g.fifth()
    scores(0, 1536, 768, 1024)
    for name in ("xA2", "xB2", "lPB2", "yA2"):
        arrived("c" + name)
    scores(1536, 2048, 0, 1024)

    def q_index(r, s, t):
        yb = bit if s == 0 else 1 - bit
        return ((x + r) % RING) * 4 + yb * 2 + (c if t == 0 else 1 - c)

    def p_index(r, s):
        yb = bit if s == 0 else 1 - bit
        return ((z + r) % RING) * 2 + yb

    for k, place in enumerate(ORDER):
        col = jnp.sum(cacc[:, pl.ds(k * ROWS, ROWS)], axis=0, keepdims=True)
        col_tx[pl.ds(p_index(*place), 1), :] = col
    for r, s in p_peers:
        send(f"col{r}{s}", col_tx, col_rx.at[(-r % RING) * 2 + s], p_device(r, s))
    for k, (place, t) in enumerate([(o, t) for o in ORDER for t in range(2)]):
        turned = jnp.transpose(racc[pl.ds(k * ROWS, ROWS), :])
        row_tx[pl.ds(q_index(*place, t), 1), :] = jnp.sum(turned, axis=0, keepdims=True)
    for r, s, t in q_peers:
        slot = (-r % RING) * 4 + s * 2 + t
        send(f"row{r}{s}{t}", row_tx, row_rx.at[slot], q_device(r, s, t))

    for peer in p_peers:
        arrived("col%d%d" % peer)
    total = col_tx[...]
    for i in range(1, 8):
        total = total + col_rx[i]
    col_inverse = 1.0 / total
    col_tot[pl.ds(0, 8), :] = col_inverse
    for peer in q_peers:
        arrived("pos%d%d%d" % peer)
    for peer in q_peers:
        arrived("row%d%d%d" % peer)
    total = row_tx[...]
    for i in range(1, 16):
        total = total + row_rx[i]
    row_tot[pl.ds(0, 16), :] = 1.0 / total
    for k, (place, t) in enumerate([(o, t) for o in ORDER for t in range(2)]):
        row_tot[pl.ds(16 + k, 1), :] = row_tot[pl.ds(q_index(*place, t), 1), :]
    for k, place in enumerate(ORDER):
        col_tot[pl.ds(8 + k, 1), :] = col_tot[pl.ds(p_index(*place), 1), :]

    def column_base(place):
        r, s = place
        zz, yy = (z + r) % RING, y if s == 0 else 3 - y
        return (team * 16 + zz * RING + yy) * ROWS

    bases = [column_base(place).astype(F32) for place in ORDER]

    def weights(first, last):
        @pl.loop(first, last)
        def _(k):
            rows = pl.ds(pl.multiple_of(k * ROWS, ROWS), ROWS)
            row_inverse = jnp.transpose(jnp.broadcast_to(row_tot[pl.ds(16 + k, 1), :], (128, 128)))
            target = jnp.transpose(
                jnp.broadcast_to(pos_buf[k, pl.ds(0, 1), :].astype(F32), (128, 128))
            )
            lane = lax.broadcasted_iota(jnp.int32, (ROWS, 128), 1).astype(F32)
            shifted = target - lane
            for j in range(8):
                cols = pl.ds(j * 128, 128)
                w = e_ref[rows, cols] * (row_inverse + col_tot[pl.ds(8 + j, 1), :])
                w = w - jnp.where(shifted == bases[j], 2.0, 0.0)
                w_ref[rows, cols] = w.astype(BF16)

    def q_dot(g):
        rows = pl.ds(g * 512, 512)
        for j in range(0, D, 256):
            cols = pl.ds(j, 256)
            qpart[rows, cols] = jnp.dot(
                w_ref[rows, :], pbuf[:, cols], preferred_element_type=F32
            ).astype(BF16)
        for k in (2 * g, 2 * g + 1):
            send(f"d{k}", qpart.at[pl.ds(k * 256 + ROWS, ROWS), :], q_d2d.at[k], sibling)

    def p_dot(g):
        out = pl.ds(g * 256, 256)
        for j in range(0, D, 256):
            cols = pl.ds(j, 256)
            ppart[out, cols] = lax.dot_general(
                w_ref[:, out],
                qbuf[:, cols],
                (((0,), (0,)), ((), ())),
                preferred_element_type=F32,
            ).astype(BF16)

    class Reduce:
        def __init__(self, tag, part, stride, extra, rx, right, left, pair):
            self.tag, self.part, self.stride, self.extra, self.rx = tag, part, stride, extra, rx
            self.to = {"x": right, "l": left, "y": pair}
            self.slots = {}

        def rows(self, place, half):
            return pl.ds(PLACE[place] * self.stride + half * HALF, HALF)

        def total(self, place, half, names):
            value = self.part[self.rows(place, half), :].astype(F32)
            if self.extra is not None:
                value += self.extra[PLACE[place], pl.ds(half * HALF, HALF), :].astype(F32)
            for name in names:
                arrived(self.tag + name)
                value += self.rx[self.slots[name]].astype(F32)
            return value

        def send(self, name, place, half, *names):
            if names or self.extra is not None:
                self.part[self.rows(place, half), :] = self.total(place, half, names).astype(BF16)
            self.slots[name] = slot = len(self.slots)
            src = self.part.at[self.rows(place, half), :]
            send(self.tag + name, src, self.rx.at[slot], self.to[name[0]])

        def one(self):
            self.send("xB0o", (2, 0), B)
            self.send("lB1o", (2, 1), B)
            self.send("yA2", (2, 1), A)

        def two(self):
            self.send("xB1r", (1, 1), B)
            self.send("yA1", (1, 1), A)
            self.send("yA3", (3, 1), A)

        def three(self):
            self.send("lB0l", (3, 0), B)
            self.send("xAo", (2, 0), A, "yA2")

        def four(self):
            self.send("yA0", (0, 1), A)
            self.send("lB1l", (3, 1), B, "lB1o")
            self.send("xB0r", (1, 0), B, "xB0o")

        def five(self):
            self.send("lAl", (3, 0), A, "yA3")
            self.send("yB1f", (0, 1), B, "xB1r", "lB1l")
            self.send("xAr", (1, 0), A, "yA1", "xAo")

        def finish(self, unit_ref, length_ref, out_ref):
            for half, names in ((B, ("xB0r", "lB0l", "yB1f")), (A, ("yA0", "lAl", "xAr"))):
                rows = pl.ds(half * HALF, HALF)
                raw = self.total((0, 0), half, names) * SCALE
                unit = unit_ref[rows, :]
                along = jnp.sum(unit * raw, axis=1, keepdims=True)
                out_ref[rows, :] = (raw - unit * along) / length_ref[rows, 0:1]

    qr = Reduce(
        "Q", qpart, 256, q_d2d, q_rx, q_device(1, 0, 0), q_device(3, 0, 0), q_device(0, 1, 0)
    )
    pr = Reduce("P", ppart, 128, None, p_rx, p_device(1, 0), p_device(3, 0), p_device(0, 1))

    def shared(*places):
        for k in places:
            arrived(f"d{k}")

    weights(12, 16)
    q_dot(3)
    weights(0, 12)
    shared(6, 7)
    qr.one()
    p_dot(3)
    pr.one()
    q_dot(2)
    p_dot(2)
    pr.two()
    shared(4, 5)
    qr.two()
    q_dot(1)
    p_dot(1)
    shared(2, 3)
    qr.three()
    pr.three()
    q_dot(0)
    p_dot(0)
    shared(0, 1)
    qr.four()
    pr.four()
    qr.five()
    pr.five()
    qr.finish(qf, q_len, qf)
    store_q = pltpu.make_async_copy(qf, gq_hbm, local_sem.at[0])
    store_q.start()
    pr.finish(pf, p_len, pf)
    store_p = pltpu.make_async_copy(pf, gp_hbm, local_sem.at[1])
    store_p.start()
    links.drain()
    store_q.wait()
    store_p.wait()


def per_device(queries, passages, positive):
    vmem = pltpu.VMEM
    anywhere = pl.BlockSpec(memory_space=pl.ANY)
    scratch = [
        vmem((ROWS, D), F32),
        vmem((ROWS, D), F32),
        vmem((ROWS, 128), F32),
        vmem((ROWS, 128), F32),
        vmem((NQ, D), BF16),
        vmem((NP, D), BF16),
        vmem((16, 8, 128), jnp.int32),
        vmem((NQ, NP), F32),
        vmem((NQ, NP), BF16),
        vmem((NQ, 128), F32),
        vmem((8, NP), F32),
        vmem((16, 128), F32),
        vmem((16, 16, 128), F32),
        vmem((8, 128), F32),
        vmem((8, 8, 128), F32),
        vmem((32, 128), F32),
        vmem((16, 128), F32),
        vmem((NQ, D), BF16),
        vmem((NP, D), BF16),
        vmem((8, ROWS, D), BF16),
        vmem((14, HALF, D), BF16),
        vmem((14, HALF, D), BF16),
        pltpu.SemaphoreType.DMA((2,)),
        pltpu.SemaphoreType.DMA((COPIES,)),
        pltpu.SemaphoreType.DMA((COPIES,)),
    ]
    out = jax.ShapeDtypeStruct((ROWS, D), F32)
    return pl.pallas_call(
        kernel,
        out_shape=(out, out),
        in_specs=[anywhere, anywhere, pl.BlockSpec(memory_space=pltpu.VMEM)],
        out_specs=(anywhere, anywhere),
        scratch_shapes=scratch,
        compiler_params=pltpu.CompilerParams(
            collective_id=0, has_side_effects=True, vmem_limit_bytes=60 << 20
        ),
    )(queries, passages, positive.reshape(1, ROWS))


def solution(mesh):
    rows = P(("team", "inner"), None)
    return jax.shard_map(
        per_device,
        mesh=mesh,
        in_specs=(rows, rows, P(("team", "inner"))),
        out_specs=(rows, rows),
        check_vma=False,
    )
```

```python
import math

import jax
import jax.numpy as jnp
from jax import lax
from jax.experimental import pallas as pl
from jax.experimental.pallas import tpu as pltpu
from jax.sharding import PartitionSpec as P

MESH = pl.DeviceIdType.MESH
F32 = jnp.float32
BF16 = jnp.bfloat16

SCALE = 20.0
EXP2_SCALE = SCALE * math.log2(math.e)
EPSILON = 1e-06
RING = 4
ROWS = 128
HALF = 64
D = 1024
NQ = 2048
NP = 1024

PLACE = {
    (0, 0): 0, (0, 1): 1, (3, 0): 2, (1, 0): 3,
    (3, 1): 4, (1, 1): 5, (2, 0): 6, (2, 1): 7,
}
ORDER = sorted(PLACE, key=PLACE.get)
A, B = 0, 1
SEMAPHORES = 75


def q_row(place, t):
    k = PLACE[place]
    return t * 512 + k * ROWS if k < 4 else k // 2 * 512 + t * 256 + k % 2 * ROWS


class Links:
    def __init__(self, semaphores, device):
        self.semaphores, self.device = semaphores, device
        self.index, self.copies = {}, {}

    def semaphore(self, name):
        i = self.index.setdefault(name, len(self.index))
        assert i < SEMAPHORES
        return self.semaphores.at[i]

    def copy(self, src, dst, sent, landed, device):
        return pltpu.make_async_remote_copy(
            src_ref=src,
            dst_ref=dst,
            send_sem=self.semaphore("sent " + sent),
            recv_sem=self.semaphore("landed " + landed),
            device_id=device,
            device_id_type=MESH,
        )

    def send(self, name, src, dst, device, sent, landed=None):
        copy = self.copy(src, dst, sent, landed or name, device)
        copy.start()
        assert name not in self.copies
        self.copies[name] = copy

    def arrived(self, name):
        self.copies[name].wait_recv()

    def all_arrived(self, landed, like):
        self.copy(like, like, "c", landed, self.device).wait_recv()

    def all_sent(self, sent, like):
        self.copy(like, like, sent, "c1", self.device).wait_send()


def kernel(
    q_hbm, p_hbm, pos_in, q_out, p_out,
    qf, pf, q_len, p_len, qbuf, pbuf, pos_buf, e_ref, w_ref, racc, cacc,
    row_tx, row_rx, col_tx, col_rx, row_tot, col_tot, qpart, ppart, q_d2d, q_rx, p_rx,
    local_sem, copy_sem,
):
    team, inner = lax.axis_index("team"), lax.axis_index("inner")
    x, c = team // 2, team % 2
    z, y = inner // RING, inner % RING
    bit = y % 2

    def device(x, y, z, c):
        return {"team": x * 2 + c, "inner": z * RING + y}

    def q_device(r, s, t):
        yy = y if s == 0 else y + 1 - 2 * bit
        return device((x + r) % RING, yy, z, c if t == 0 else 1 - c)

    def p_device(r, s):
        return device(x, y if s == 0 else 3 - y, (z + r) % RING, c)

    q_peers = [(r, s, t) for r in range(RING) for s in range(2) for t in range(2)][1:]
    p_peers = [(r, s) for r in range(RING) for s in range(2)][1:]

    loads = [
        pltpu.make_async_copy(q_hbm, qf, local_sem.at[0]),
        pltpu.make_async_copy(p_hbm, pf, local_sem.at[1]),
    ]
    for load in loads:
        load.start()
    barrier = pltpu.get_barrier_semaphore()
    neighbours = [q_device(*peer) for peer in ((1, 0, 0), (3, 0, 0), (0, 1, 0), (0, 0, 1))]
    neighbours += [p_device(*peer) for peer in ((1, 0), (3, 0), (0, 1))]
    for neighbour in neighbours:
        pl.semaphore_signal(barrier, inc=1, device_id=neighbour, device_id_type=MESH)

    sibling = q_device(0, 0, 1)
    links = Links(copy_sem, sibling)
    send, arrived = links.send, links.arrived

    def normalize(full, length_ref, rounded):
        v = full[...]
        length = jnp.sqrt(jnp.sum(v * v, axis=1, keepdims=True) + EPSILON)
        unit = v / length
        full[...] = unit
        length_ref[...] = jnp.broadcast_to(length, (ROWS, 128))
        rounded[pl.ds(0, ROWS), :] = unit.astype(BF16)

    loads[0].wait()
    normalize(qf, q_len, qbuf)
    loads[1].wait()
    normalize(pf, p_len, pbuf)
    pos_buf[0] = jnp.broadcast_to(pos_in[...], (8, 128))
    racc[...] = jnp.zeros_like(racc)
    cacc[...] = jnp.zeros_like(cacc)
    pl.semaphore_wait(barrier, len(neighbours))

    def q_at(place, half, t=0):
        return qbuf.at[pl.ds(q_row(place, t) + half * HALF, HALF), :]

    def p_at(place, half):
        return pbuf.at[pl.ds(PLACE[place] * ROWS + half * HALF, HALF), :]

    class Gather:
        def __init__(self, tag, at, right, left, pair, on_arrival):
            self.tag, self.at, self.on_arrival = tag, at, on_arrival
            self.to = {"x": right, "l": left, "y": pair}
            self.landed = {}

        def send(self, name, src, dst, half):
            self.landed[name] = (dst, half)
            send(self.tag + name, self.at(src, half), self.at(dst, half), self.to[name[0]], self.tag)

        def take(self, name):
            arrived(self.tag + name)
            self.on_arrival(name, *self.landed[name])

        def begin(self):
            self.send("xA", (0, 0), (3, 0), A)
            self.send("lA", (0, 0), (1, 0), A)
            self.send("yB", (0, 0), (0, 1), B)
            self.send("xB", (0, 0), (3, 0), B)
            self.send("lB", (0, 0), (1, 0), B)
            self.send("yA", (0, 0), (0, 1), A)

        def first(self):
            self.take("xA")
            self.send("xA2", (3, 0), (2, 0), A)
            self.send("yA3", (3, 0), (3, 1), A)
            self.take("lA")
            self.send("yA1", (1, 0), (1, 1), A)
            self.take("yB")
            self.send("xPB", (0, 1), (3, 1), B)
            self.send("lPB", (0, 1), (1, 1), B)

        def second(self):
            self.take("xB")
            self.send("xB2", (3, 0), (2, 0), B)
            self.take("lB")
            self.take("yA")

        def third(self):
            self.take("lPB")
            self.send("lPB2", (1, 1), (2, 1), B)
            self.take("xA2")
            self.send("yA2", (2, 0), (2, 1), A)
            self.take("yA3")

        def fourth(self):
            self.take("xPB")
            self.take("yA1")

        def fifth(self):
            self.take("xB2")
            self.take("lPB2")
            self.take("yA2")

    def share(name, place, half):
        stage = "c1" if PLACE[place] < 4 else "c2" if PLACE[place] < 6 else "c3"
        send("c" + name, q_at(place, half, 0), q_at(place, half, 1), sibling, "c", stage)

    qg = Gather("q", q_at, q_device(1, 0, 0), q_device(3, 0, 0), q_device(0, 1, 0), share)
    pg = Gather("p", p_at, p_device(1, 0), p_device(3, 0), p_device(0, 1), lambda *_: None)
    qg.begin()
    pg.begin()
    send("c", qbuf.at[pl.ds(0, ROWS), :], qbuf.at[pl.ds(512, ROWS), :], sibling, "c", "c1")

    def scores(rows0, rows1, cols0, cols1, step=512):
        width = 256

        @pl.loop(0, (rows1 - rows0) // step)
        def _(i):
            rows = pl.ds(pl.multiple_of(rows0 + i * step, step), step)
            for j in range(cols0, cols1, width):
                cols = pl.ds(j, width)
                s = lax.dot_general(
                    qbuf[rows, :],
                    pbuf[cols, :],
                    (((1,), (1,)), ((), ())),
                    preferred_element_type=F32,
                )
                e = jnp.exp2(s * EXP2_SCALE)
                e_ref[rows, cols] = e
                part = e[:, 0:128]
                for k in range(128, width, 128):
                    part = part + e[:, k : k + 128]
                racc[rows, :] += part
                cacc[:, cols] += jnp.sum(e.reshape(step // 8, 8, width), axis=0)

    def landed(stage, rows, count):
        links.all_arrived(stage, qbuf.at[pl.ds(rows, count), :])

    for g in (qg, pg):
        g.first()
    for g in (qg, pg):
        g.second()
    scores(0, 512, 0, 512)
    landed("c1", 512, 512)
    scores(512, 1024, 0, 512)
    for g in (qg, pg):
        g.third()
    for g in (qg, pg):
        g.fourth()
    scores(0, 1024, 512, 768)
    scores(1024, 1280, 0, 768, 256)
    landed("c2", 1280, 256)
    scores(1280, 1536, 0, 768, 256)
    for g in (qg, pg):
        g.fifth()
    blocks = [(place, t) for place in ORDER for t in range(2)]
    for r, s, t in q_peers:
        slot = q_row((-r % RING, s), t) // ROWS
        send(f"pos{r}{s}{t}", pos_buf.at[0], pos_buf.at[slot], q_device(r, s, t), "pos", "pos")
    scores(0, 1536, 768, 1024)
    scores(1536, 1792, 0, 1024, 256)
    landed("c3", 1792, 256)
    scores(1792, 2048, 0, 1024, 256)

    def q_index(r, s, t):
        yb = bit if s == 0 else 1 - bit
        return ((x + r) % RING) * 4 + yb * 2 + (c if t == 0 else 1 - c)

    def p_index(r, s):
        yb = bit if s == 0 else 1 - bit
        return ((z + r) % RING) * 2 + yb

    for k, place in enumerate(ORDER):
        col = jnp.sum(cacc[:, pl.ds(k * ROWS, ROWS)], axis=0, keepdims=True)
        col_tx[pl.ds(p_index(*place), 1), :] = col
    for r, s in p_peers:
        slot = (-r % RING) * 2 + s
        send(f"col{r}{s}", col_tx, col_rx.at[slot], p_device(r, s), "col", "col")
    for place, t in blocks:
        turned = jnp.transpose(racc[pl.ds(q_row(place, t), ROWS), :])
        row_tx[pl.ds(q_index(*place, t), 1), :] = jnp.sum(turned, axis=0, keepdims=True)
    for r, s, t in q_peers:
        slot = (-r % RING) * 4 + s * 2 + t
        send(f"row{r}{s}{t}", row_tx, row_rx.at[slot], q_device(r, s, t), "row", "row")

    links.all_arrived("col", col_rx.at[pl.ds(1, 7)])
    total = col_tx[...]
    for i in range(1, 8):
        total = total + col_rx[i]
    col_inverse = 1.0 / total
    col_tot[pl.ds(0, 8), :] = col_inverse
    links.all_arrived("pos", pos_buf.at[pl.ds(1, 15)])
    links.all_arrived("row", row_rx.at[pl.ds(1, 15)])
    total = row_tx[...]
    for i in range(1, 16):
        total = total + row_rx[i]
    row_tot[pl.ds(0, 16), :] = 1.0 / total
    for place, t in blocks:
        row_tot[pl.ds(16 + q_row(place, t) // ROWS, 1), :] = row_tot[pl.ds(q_index(*place, t), 1), :]
    for k, place in enumerate(ORDER):
        col_tot[pl.ds(8 + k, 1), :] = col_tot[pl.ds(p_index(*place), 1), :]

    def column_base(place):
        r, s = place
        zz, yy = (z + r) % RING, y if s == 0 else 3 - y
        return (team * 16 + zz * RING + yy) * ROWS

    bases = [column_base(place).astype(F32) for place in ORDER]

    def weights(first, last, cols0, cols1):
        @pl.loop(first, last)
        def _(k):
            rows = pl.ds(pl.multiple_of(k * ROWS, ROWS), ROWS)
            row_inverse = jnp.transpose(jnp.broadcast_to(row_tot[pl.ds(16 + k, 1), :], (128, 128)))
            target = jnp.transpose(
                jnp.broadcast_to(pos_buf[k, pl.ds(0, 1), :].astype(F32), (128, 128))
            )
            lane = lax.broadcasted_iota(jnp.int32, (ROWS, 128), 1).astype(F32)
            shifted = target - lane
            for j in range(cols0, cols1):
                cols = pl.ds(j * 128, 128)
                w = e_ref[rows, cols] * (row_inverse + col_tot[pl.ds(8 + j, 1), :])
                w = w - jnp.where(shifted == bases[j], 2.0, 0.0)
                w_ref[rows, cols] = w.astype(BF16)

    def q_dot(first, last):
        rows = pl.ds(first, last - first)
        for j in range(0, D, 256):
            cols = pl.ds(j, 256)
            qpart[rows, cols] = jnp.dot(
                w_ref[rows, :], pbuf[:, cols], preferred_element_type=F32
            ).astype(BF16)

    def q_dots(own, other, blocks, shared_first):
        q_dot(other, other + blocks * ROWS)
        rows = blocks * ROWS
        send(
            f"d{shared_first}",
            qpart.at[pl.ds(other, rows), :],
            q_d2d.at[pl.ds(shared_first, rows), :],
            sibling,
            "d",
        )
        q_dot(own, own + rows)

    def p_dot(first, last):
        out = pl.ds(first, last - first)
        for j in range(0, D, 256):
            cols = pl.ds(j, 256)
            ppart[out, cols] = lax.dot_general(
                w_ref[:, out],
                qbuf[:, cols],
                (((0,), (0,)), ((), ())),
                preferred_element_type=F32,
            ).astype(BF16)

    class Reduce:
        def __init__(self, tag, part, row, extra, rx, right, left, pair):
            self.tag, self.part, self.row, self.extra, self.rx = tag, part, row, extra, rx
            self.to = {"x": right, "l": left, "y": pair}
            self.slots = {}

        def rows(self, place, half):
            return pl.ds(self.row(place) + half * HALF, HALF)

        def total(self, place, half, names):
            value = self.part[self.rows(place, half), :].astype(F32)
            if self.extra is not None:
                rows = pl.ds(PLACE[place] * ROWS + half * HALF, HALF)
                value += self.extra[rows, :].astype(F32)
            for name in names:
                arrived(self.tag + name)
                value += self.rx[self.slots[name]].astype(F32)
            return value

        def send(self, name, place, half, *names):
            if names or self.extra is not None:
                self.part[self.rows(place, half), :] = self.total(place, half, names).astype(BF16)
            self.slots[name] = slot = len(self.slots)
            src = self.part.at[self.rows(place, half), :]
            send(self.tag + name, src, self.rx.at[slot], self.to[name[0]], self.tag)

        def one(self):
            self.send("xB0o", (2, 0), B)
            self.send("lB1o", (2, 1), B)
            self.send("yA2", (2, 1), A)

        def two(self):
            self.send("xB1r", (1, 1), B)
            self.send("yA1", (1, 1), A)
            self.send("yA3", (3, 1), A)

        def three(self):
            self.send("lB1l", (3, 1), B, "lB1o")
            self.send("xAo", (2, 0), A, "yA2")

        def four(self):
            self.send("lB0l", (3, 0), B)
            self.send("xB0r", (1, 0), B, "xB0o")
            self.send("yA0", (0, 1), A)

        def five(self):
            self.send("yB1f", (0, 1), B, "xB1r", "lB1l")

        def six(self):
            self.send("lAl", (3, 0), A, "yA3")
            self.send("xAr", (1, 0), A, "yA1", "xAo")

        def finish(self, unit_ref, length_ref, out_ref):
            for half, names in ((B, ("xB0r", "lB0l", "yB1f")), (A, ("yA0", "lAl", "xAr"))):
                rows = pl.ds(half * HALF, HALF)
                raw = self.total((0, 0), half, names) * SCALE
                unit = unit_ref[rows, :]
                along = jnp.sum(unit * raw, axis=1, keepdims=True)
                out_ref[rows, :] = (raw - unit * along) / length_ref[rows, 0:1]

    qr = Reduce(
        "Q", qpart, lambda place: q_row(place, 0), q_d2d, q_rx,
        q_device(1, 0, 0), q_device(3, 0, 0), q_device(0, 1, 0),
    )
    pr = Reduce(
        "P", ppart, lambda place: PLACE[place] * ROWS, None, p_rx,
        p_device(1, 0), p_device(3, 0), p_device(0, 1),
    )

    weights(12, 16, 0, 8)
    q_dots(1536, 1792, 2, 768)
    weights(0, 12, 6, 8)
    arrived("d768")
    qr.one()
    p_dot(768, 1024)
    pr.one()
    weights(8, 12, 0, 6)
    q_dots(1024, 1280, 2, 512)
    weights(0, 8, 4, 6)
    arrived("d512")
    qr.two()
    p_dot(512, 768)
    pr.two()
    qr.three()
    weights(0, 8, 0, 4)
    q_dots(128, 640, 3, 128)
    pr.three()
    arrived("d128")
    qr.four()
    p_dot(128, 512)
    pr.four()
    qr.five()
    q_dots(0, 512, 1, 0)
    qr.six()
    p_dot(0, 128)
    pr.five()
    pr.six()
    arrived("d0")
    qr.finish(qf, q_len, q_out)
    pr.finish(pf, p_len, p_out)
    for sent, like in (
        ("q", q_rx), ("p", p_rx), ("Q", q_rx), ("P", p_rx),
        ("c", q_d2d), ("d", q_d2d),
        ("pos", pos_buf.at[pl.ds(1, 15)]),
        ("row", row_rx.at[pl.ds(1, 15)]),
        ("col", col_rx.at[pl.ds(1, 7)]),
    ):
        links.all_sent(sent, like)


def put_out(q_in, p_in, q_hbm, p_hbm, sem):
    copies = [
        pltpu.make_async_copy(q_in, q_hbm, sem.at[0]),
        pltpu.make_async_copy(p_in, p_hbm, sem.at[1]),
    ]
    for copy in copies:
        copy.start()
    for copy in copies:
        copy.wait()


def per_device(queries, passages, positive):
    vmem = pltpu.VMEM
    scratch = [
        vmem((ROWS, D), F32),
        vmem((ROWS, D), F32),
        vmem((ROWS, 128), F32),
        vmem((ROWS, 128), F32),
        vmem((NQ, D), BF16),
        vmem((NP, D), BF16),
        vmem((16, 8, 128), jnp.int32),
        vmem((NQ, NP), F32),
        vmem((NQ, NP), BF16),
        vmem((NQ, 128), F32),
        vmem((8, NP), F32),
        vmem((16, 128), F32),
        vmem((16, 16, 128), F32),
        vmem((8, 128), F32),
        vmem((8, 8, 128), F32),
        vmem((32, 128), F32),
        vmem((16, 128), F32),
        vmem((NQ, D), BF16),
        vmem((NP, D), BF16),
        vmem((1024, D), BF16),
        vmem((14, HALF, D), BF16),
        vmem((14, HALF, D), BF16),
        pltpu.SemaphoreType.DMA((2,)),
        pltpu.SemaphoreType.DMA((SEMAPHORES,)),
    ]
    out = jax.ShapeDtypeStruct((ROWS, D), F32)
    here = pl.BlockSpec(memory_space=pltpu.VMEM)
    hbm = pl.BlockSpec(memory_space=pltpu.HBM)
    grads = pl.pallas_call(
        kernel,
        out_shape=(out, out),
        in_specs=[hbm, hbm, here],
        out_specs=(here, here),
        scratch_shapes=scratch,
        compiler_params=pltpu.CompilerParams(
            collective_id=0, has_side_effects=True, vmem_limit_bytes=56 << 20
        ),
    )(queries, passages, positive.reshape(1, ROWS))
    return pl.pallas_call(
        put_out,
        out_shape=(out, out),
        in_specs=[here, here],
        out_specs=(hbm, hbm),
        scratch_shapes=[pltpu.SemaphoreType.DMA((2,))],
        compiler_params=pltpu.CompilerParams(vmem_limit_bytes=1 << 20),
    )(*grads)


def solution(mesh):
    rows = P(("team", "inner"), None)
    return jax.shard_map(
        per_device,
        mesh=mesh,
        in_specs=(rows, rows, P(("team", "inner"))),
        out_specs=(rows, rows),
        check_vma=False,
    )
```

```python
import math

import jax
import jax.numpy as jnp
from jax import lax
from jax.experimental import pallas as pl
from jax.experimental.pallas import tpu as pltpu
from jax.sharding import PartitionSpec as P

MESH = pl.DeviceIdType.MESH
F32 = jnp.float32
BF16 = jnp.bfloat16

SCALE = 20.0
EXP2_SCALE = SCALE * math.log2(math.e)
EPSILON = 1e-06
RING = 4
ROWS = 128
HALF = 64
D = 1024
NQ = 2048
NP = 1024

PLACE = {
    (0, 0): 0, (0, 1): 1, (3, 0): 2, (1, 0): 3,
    (3, 1): 4, (1, 1): 5, (2, 0): 6, (2, 1): 7,
}
ORDER = sorted(PLACE, key=PLACE.get)
A, B = 0, 1
SEMAPHORES = 75


def q_row(place, t):
    k = PLACE[place]
    return t * 512 + k * ROWS if k < 4 else k // 2 * 512 + t * 256 + k % 2 * ROWS


class Links:
    def __init__(self, semaphores, device):
        self.semaphores, self.device = semaphores, device
        self.index, self.copies = {}, {}

    def semaphore(self, name):
        i = self.index.setdefault(name, len(self.index))
        assert i < SEMAPHORES
        return self.semaphores.at[i]

    def copy(self, src, dst, sent, landed, device):
        return pltpu.make_async_remote_copy(
            src_ref=src,
            dst_ref=dst,
            send_sem=self.semaphore("sent " + sent),
            recv_sem=self.semaphore("landed " + landed),
            device_id=device,
            device_id_type=MESH,
        )

    def send(self, name, src, dst, device, sent, landed=None):
        copy = self.copy(src, dst, sent, landed or name, device)
        copy.start()
        assert name not in self.copies
        self.copies[name] = copy

    def arrived(self, name):
        self.copies[name].wait_recv()

    def all_arrived(self, landed, like):
        self.copy(like, like, "c", landed, self.device).wait_recv()

    def all_sent(self, sent, like):
        self.copy(like, like, sent, "c1", self.device).wait_send()


def kernel(
    q_hbm, p_hbm, pos_in, q_out, p_out,
    qf, pf, q_len, p_len, qbuf, pbuf, pos_buf, e_ref, w_ref, racc, cacc,
    row_tx, row_rx, col_tx, col_rx, row_tot, col_tot, qpart, ppart, q_d2d, q_rx, p_rx,
    shifted, row_inverse, local_sem, copy_sem,
):
    team, inner = lax.axis_index("team"), lax.axis_index("inner")
    x, c = team // 2, team % 2
    z, y = inner // RING, inner % RING
    bit = y % 2

    def device(x, y, z, c):
        return {"team": x * 2 + c, "inner": z * RING + y}

    def q_device(r, s, t):
        yy = y if s == 0 else y + 1 - 2 * bit
        return device((x + r) % RING, yy, z, c if t == 0 else 1 - c)

    def p_device(r, s):
        return device(x, y if s == 0 else 3 - y, (z + r) % RING, c)

    q_peers = [(r, s, t) for r in range(RING) for s in range(2) for t in range(2)][1:]
    p_peers = [(r, s) for r in range(RING) for s in range(2)][1:]

    loads = [
        pltpu.make_async_copy(q_hbm, qf, local_sem.at[0]),
        pltpu.make_async_copy(p_hbm, pf, local_sem.at[1]),
    ]
    for load in loads:
        load.start()
    barrier = pltpu.get_barrier_semaphore()
    neighbours = [q_device(*peer) for peer in ((1, 0, 0), (3, 0, 0), (0, 1, 0), (0, 0, 1))]
    neighbours += [p_device(*peer) for peer in ((1, 0), (3, 0), (0, 1))]
    for neighbour in neighbours:
        pl.semaphore_signal(barrier, inc=1, device_id=neighbour, device_id_type=MESH)

    sibling = q_device(0, 0, 1)
    links = Links(copy_sem, sibling)
    send, arrived = links.send, links.arrived

    def normalize(full, length_ref, rounded):
        v = full[...]
        length = jnp.sqrt(jnp.sum(v * v, axis=1, keepdims=True) + EPSILON)
        unit = v / length
        full[...] = unit
        length_ref[...] = jnp.broadcast_to(length, (ROWS, 128))
        rounded[pl.ds(0, ROWS), :] = unit.astype(BF16)

    loads[0].wait()
    normalize(qf, q_len, qbuf)
    loads[1].wait()
    normalize(pf, p_len, pbuf)
    pos_buf[0] = jnp.broadcast_to(pos_in[...], (8, 128))
    racc[...] = jnp.zeros_like(racc)
    cacc[...] = jnp.zeros_like(cacc)
    pl.semaphore_wait(barrier, len(neighbours))

    def q_at(place, half, t=0):
        return qbuf.at[pl.ds(q_row(place, t) + half * HALF, HALF), :]

    def p_at(place, half):
        return pbuf.at[pl.ds(PLACE[place] * ROWS + half * HALF, HALF), :]

    class Gather:
        def __init__(self, tag, at, right, left, pair, on_arrival):
            self.tag, self.at, self.on_arrival = tag, at, on_arrival
            self.to = {"x": right, "l": left, "y": pair}
            self.landed = {}

        def send(self, name, src, dst, half):
            self.landed[name] = (dst, half)
            send(self.tag + name, self.at(src, half), self.at(dst, half), self.to[name[0]], self.tag)

        def take(self, name):
            arrived(self.tag + name)
            self.on_arrival(name, *self.landed[name])

        def begin(self):
            self.send("xA", (0, 0), (3, 0), A)
            self.send("lA", (0, 0), (1, 0), A)
            self.send("yB", (0, 0), (0, 1), B)
            self.send("xB", (0, 0), (3, 0), B)
            self.send("lB", (0, 0), (1, 0), B)
            self.send("yA", (0, 0), (0, 1), A)

        def first(self):
            self.take("xA")
            self.send("xA2", (3, 0), (2, 0), A)
            self.send("yA3", (3, 0), (3, 1), A)
            self.take("lA")
            self.send("yA1", (1, 0), (1, 1), A)
            self.take("yB")
            self.send("xPB", (0, 1), (3, 1), B)
            self.send("lPB", (0, 1), (1, 1), B)

        def second(self):
            self.take("xB")
            self.send("xB2", (3, 0), (2, 0), B)
            self.take("lB")
            self.take("yA")

        def third(self):
            self.take("lPB")
            self.send("lPB2", (1, 1), (2, 1), B)
            self.take("xA2")
            self.send("yA2", (2, 0), (2, 1), A)
            self.take("yA3")

        def fourth(self):
            self.take("xPB")
            self.take("yA1")

        def fifth(self):
            self.take("xB2")
            self.take("lPB2")
            self.take("yA2")

    def share(name, place, half):
        stage = "c1" if PLACE[place] < 4 else "c2" if PLACE[place] < 6 else "c3"
        send("c" + name, q_at(place, half, 0), q_at(place, half, 1), sibling, "c", stage)

    qg = Gather("q", q_at, q_device(1, 0, 0), q_device(3, 0, 0), q_device(0, 1, 0), share)
    pg = Gather("p", p_at, p_device(1, 0), p_device(3, 0), p_device(0, 1), lambda *_: None)
    qg.begin()
    pg.begin()
    send("c", qbuf.at[pl.ds(0, ROWS), :], qbuf.at[pl.ds(512, ROWS), :], sibling, "c", "c1")

    def scores(rows0, rows1, cols0, cols1, step=512):
        width = 256
        for i in range(rows0, rows1, step):
            rows = pl.ds(i, step)
            for j in range(cols0, cols1, width):
                cols = pl.ds(j, width)
                s = lax.dot_general(
                    qbuf[rows, :],
                    pbuf[cols, :],
                    (((1,), (1,)), ((), ())),
                    preferred_element_type=F32,
                )
                e = jnp.exp2(s * EXP2_SCALE)
                e_ref[rows, cols] = e
                part = e[:, 0:128]
                for k in range(128, width, 128):
                    part = part + e[:, k : k + 128]
                racc[rows, :] += part
                cacc[:, cols] += jnp.sum(e.reshape(step // 8, 8, width), axis=0)

    def landed(stage, rows, count):
        links.all_arrived(stage, qbuf.at[pl.ds(rows, count), :])

    for g in (qg, pg):
        g.first()
    for g in (qg, pg):
        g.second()
    scores(0, 512, 0, 512)
    landed("c1", 512, 512)
    scores(512, 1024, 0, 512)
    for g in (qg, pg):
        g.third()
    for g in (qg, pg):
        g.fourth()
    scores(0, 1024, 512, 768)
    scores(1024, 1280, 0, 768, 256)
    landed("c2", 1280, 256)
    scores(1280, 1536, 0, 768, 256)
    for g in (qg, pg):
        g.fifth()
    blocks = [(place, t) for place in ORDER for t in range(2)]
    for r, s, t in q_peers:
        slot = q_row((-r % RING, s), t) // ROWS
        send(f"pos{r}{s}{t}", pos_buf.at[0], pos_buf.at[slot], q_device(r, s, t), "pos", "pos")
    scores(0, 1536, 768, 1024)
    scores(1536, 1792, 0, 1024, 256)
    landed("c3", 1792, 256)
    scores(1792, 2048, 0, 1024, 256)

    def q_index(r, s, t):
        yb = bit if s == 0 else 1 - bit
        return ((x + r) % RING) * 4 + yb * 2 + (c if t == 0 else 1 - c)

    def p_index(r, s):
        yb = bit if s == 0 else 1 - bit
        return ((z + r) % RING) * 2 + yb

    for k, place in enumerate(ORDER):
        col = jnp.sum(cacc[:, pl.ds(k * ROWS, ROWS)], axis=0, keepdims=True)
        col_tx[pl.ds(p_index(*place), 1), :] = col
    for r, s in p_peers:
        slot = (-r % RING) * 2 + s
        send(f"col{r}{s}", col_tx, col_rx.at[slot], p_device(r, s), "col", "col")
    for place, t in blocks:
        turned = jnp.transpose(racc[pl.ds(q_row(place, t), ROWS), :])
        row_tx[pl.ds(q_index(*place, t), 1), :] = jnp.sum(turned, axis=0, keepdims=True)
    for r, s, t in q_peers:
        slot = (-r % RING) * 4 + s * 2 + t
        send(f"row{r}{s}{t}", row_tx, row_rx.at[slot], q_device(r, s, t), "row", "row")

    links.all_arrived("pos", pos_buf.at[pl.ds(1, 15)])
    lane = lax.broadcasted_iota(jnp.int32, (ROWS, 128), 1).astype(F32)
    for k in range(16):
        target = jnp.broadcast_to(pos_buf[k, pl.ds(0, 1), :].astype(F32), (128, 128))
        shifted[pl.ds(k * ROWS, ROWS), :] = jnp.transpose(target) - lane
    links.all_arrived("col", col_rx.at[pl.ds(1, 7)])
    total = col_tx[...]
    for i in range(1, 8):
        total = total + col_rx[i]
    col_inverse = 1.0 / total
    col_tot[pl.ds(0, 8), :] = col_inverse
    links.all_arrived("row", row_rx.at[pl.ds(1, 15)])
    total = row_tx[...]
    for i in range(1, 16):
        total = total + row_rx[i]
    row_tot[pl.ds(0, 16), :] = 1.0 / total
    for place, t in blocks:
        row_tot[pl.ds(16 + q_row(place, t) // ROWS, 1), :] = row_tot[pl.ds(q_index(*place, t), 1), :]
    for k, place in enumerate(ORDER):
        col_tot[pl.ds(8 + k, 1), :] = col_tot[pl.ds(p_index(*place), 1), :]

    def column_base(place):
        r, s = place
        zz, yy = (z + r) % RING, y if s == 0 else 3 - y
        return (team * 16 + zz * RING + yy) * ROWS

    bases = [column_base(place).astype(F32) for place in ORDER]

    def row_factor(k):
        rows = pl.ds(k * ROWS, ROWS)
        factor = jnp.broadcast_to(row_tot[pl.ds(16 + k, 1), :], (128, 128))
        row_inverse[rows, :] = jnp.transpose(factor)

    def weight(k, j):
        rows, cols = pl.ds(k * ROWS, ROWS), pl.ds(j * 128, 128)
        w = e_ref[rows, cols] * (row_inverse[rows, :] + col_tot[pl.ds(8 + j, 1), :])
        w = w - jnp.where(shifted[rows, :] == bases[j], 2.0, 0.0)
        w_ref[rows, cols] = w.astype(BF16)

    def weights(slots, cols):
        return [(weight, k, j) for k in slots for j in cols]

    def run(work):
        for f, *args in work:
            f(*args)

    def q_dot(first, last, beside=()):
        rows = pl.ds(first, last - first)
        for i in range(4):
            cols = pl.ds(i * 256, 256)
            qpart[rows, cols] = jnp.dot(
                w_ref[rows, :], pbuf[:, cols], preferred_element_type=F32
            ).astype(BF16)
            run(beside[len(beside) * i // 4 : len(beside) * (i + 1) // 4])

    def q_dots(own, other, blocks, shared_first, beside=()):
        half = len(beside) // 2
        rows = blocks * ROWS
        q_dot(other, other + rows, beside[:half])
        send(
            f"d{shared_first}",
            qpart.at[pl.ds(other, rows), :],
            q_d2d.at[pl.ds(shared_first, rows), :],
            sibling,
            "d",
        )
        q_dot(own, own + rows, beside[half:])

    def p_dot(first, last, tiles=range(4), beside=()):
        out = pl.ds(first, last - first)
        for n, i in enumerate(tiles):
            cols = pl.ds(i * 256, 256)
            ppart[out, cols] = lax.dot_general(
                w_ref[:, out],
                qbuf[:, cols],
                (((0,), (0,)), ((), ())),
                preferred_element_type=F32,
            ).astype(BF16)
            run(beside[len(beside) * n // len(tiles) : len(beside) * (n + 1) // len(tiles)])

    class Reduce:
        def __init__(self, tag, part, row, extra, rx, right, left, pair):
            self.tag, self.part, self.row, self.extra, self.rx = tag, part, row, extra, rx
            self.to = {"x": right, "l": left, "y": pair}
            self.slots = {}

        def rows(self, place, half):
            return pl.ds(self.row(place) + half * HALF, HALF)

        def total(self, place, half, names):
            value = self.part[self.rows(place, half), :].astype(F32)
            if self.extra is not None:
                rows = pl.ds(PLACE[place] * ROWS + half * HALF, HALF)
                value += self.extra[rows, :].astype(F32)
            for name in names:
                arrived(self.tag + name)
                value += self.rx[self.slots[name]].astype(F32)
            return value

        def send(self, name, place, half, *names):
            if names or self.extra is not None:
                self.part[self.rows(place, half), :] = self.total(place, half, names).astype(BF16)
            self.slots[name] = slot = len(self.slots)
            src = self.part.at[self.rows(place, half), :]
            send(self.tag + name, src, self.rx.at[slot], self.to[name[0]], self.tag)

        def one(self):
            self.send("xB0o", (2, 0), B)
            self.send("lB1o", (2, 1), B)
            self.send("yA2", (2, 1), A)

        def two(self):
            self.send("xB1r", (1, 1), B)
            self.send("yA1", (1, 1), A)
            self.send("yA3", (3, 1), A)

        def three(self):
            self.send("lB1l", (3, 1), B, "lB1o")
            self.send("xAo", (2, 0), A, "yA2")

        def four(self):
            self.send("lB0l", (3, 0), B)
            self.send("xB0r", (1, 0), B, "xB0o")
            self.send("yA0", (0, 1), A)

        def five(self):
            self.send("yB1f", (0, 1), B, "xB1r", "lB1l")

        def six(self):
            self.send("lAl", (3, 0), A, "yA3")
            self.send("xAr", (1, 0), A, "yA1", "xAo")

        def finish(self, unit_ref, length_ref, out_ref):
            for half, names in ((B, ("xB0r", "lB0l", "yB1f")), (A, ("yA0", "lAl", "xAr"))):
                rows = pl.ds(half * HALF, HALF)
                raw = self.total((0, 0), half, names) * SCALE
                unit = unit_ref[rows, :]
                along = jnp.sum(unit * raw, axis=1, keepdims=True)
                out_ref[rows, :] = (raw - unit * along) / length_ref[rows, 0:1]

    qr = Reduce(
        "Q", qpart, lambda place: q_row(place, 0), q_d2d, q_rx,
        q_device(1, 0, 0), q_device(3, 0, 0), q_device(0, 1, 0),
    )
    pr = Reduce(
        "P", ppart, lambda place: PLACE[place] * ROWS, None, p_rx,
        p_device(1, 0), p_device(3, 0), p_device(0, 1),
    )

    for k in range(12, 16):
        row_factor(k)
    run(weights(range(12, 16), range(8)))
    later = [(row_factor, k) for k in range(12)] + weights(range(12), (6, 7))
    q_dots(1536, 1792, 2, 768, later)
    later = weights(range(8, 12), range(6))
    p_dot(768, 1024, (0, 1), later[:12])
    arrived("d768")
    qr.one()
    p_dot(768, 1024, (2, 3), later[12:])
    pr.one()
    q_dots(1024, 1280, 2, 512, weights(range(8), (4, 5)))
    later = weights(range(8), range(4))
    p_dot(512, 768, (0, 1), later[:16])
    arrived("d512")
    qr.two()
    p_dot(512, 768, (2, 3), later[16:])
    pr.two()
    qr.three()
    q_dots(128, 640, 3, 128)
    pr.three()
    p_dot(128, 512, (0, 1))
    arrived("d128")
    qr.four()
    p_dot(128, 512, (2, 3))
    pr.four()
    qr.five()
    q_dots(0, 512, 1, 0)
    qr.six()
    p_dot(0, 128)
    pr.five()
    pr.six()
    arrived("d0")
    qr.finish(qf, q_len, q_out)
    pr.finish(pf, p_len, p_out)
    for sent, like in (
        ("q", q_rx), ("p", p_rx), ("Q", q_rx), ("P", p_rx),
        ("c", q_d2d), ("d", q_d2d),
        ("pos", pos_buf.at[pl.ds(1, 15)]),
        ("row", row_rx.at[pl.ds(1, 15)]),
        ("col", col_rx.at[pl.ds(1, 7)]),
    ):
        links.all_sent(sent, like)


def put_out(q_in, p_in, q_hbm, p_hbm, sem):
    copies = [
        pltpu.make_async_copy(q_in, q_hbm, sem.at[0]),
        pltpu.make_async_copy(p_in, p_hbm, sem.at[1]),
    ]
    for copy in copies:
        copy.start()
    for copy in copies:
        copy.wait()


def per_device(queries, passages, positive):
    vmem = pltpu.VMEM
    scratch = [
        vmem((ROWS, D), F32),
        vmem((ROWS, D), F32),
        vmem((ROWS, 128), F32),
        vmem((ROWS, 128), F32),
        vmem((NQ, D), BF16),
        vmem((NP, D), BF16),
        vmem((16, 8, 128), jnp.int32),
        vmem((NQ, NP), F32),
        vmem((NQ, NP), BF16),
        vmem((NQ, 128), F32),
        vmem((8, NP), F32),
        vmem((16, 128), F32),
        vmem((16, 16, 128), F32),
        vmem((8, 128), F32),
        vmem((8, 8, 128), F32),
        vmem((32, 128), F32),
        vmem((16, 128), F32),
        vmem((NQ, D), BF16),
        vmem((NP, D), BF16),
        vmem((1024, D), BF16),
        vmem((14, HALF, D), BF16),
        vmem((14, HALF, D), BF16),
        vmem((NQ, 128), F32),
        vmem((NQ, 128), F32),
        pltpu.SemaphoreType.DMA((2,)),
        pltpu.SemaphoreType.DMA((SEMAPHORES,)),
    ]
    out = jax.ShapeDtypeStruct((ROWS, D), F32)
    here = pl.BlockSpec(memory_space=pltpu.VMEM)
    hbm = pl.BlockSpec(memory_space=pltpu.HBM)
    grads = pl.pallas_call(
        kernel,
        out_shape=(out, out),
        in_specs=[hbm, hbm, here],
        out_specs=(here, here),
        scratch_shapes=scratch,
        compiler_params=pltpu.CompilerParams(
            collective_id=0, has_side_effects=True, vmem_limit_bytes=52 << 20
        ),
    )(queries, passages, positive.reshape(1, ROWS))
    return pl.pallas_call(
        put_out,
        out_shape=(out, out),
        in_specs=[here, here],
        out_specs=(hbm, hbm),
        scratch_shapes=[pltpu.SemaphoreType.DMA((2,))],
        compiler_params=pltpu.CompilerParams(vmem_limit_bytes=1 << 20),
    )(*grads)


def solution(mesh):
    rows = P(("team", "inner"), None)
    return jax.shard_map(
        per_device,
        mesh=mesh,
        in_specs=(rows, rows, P(("team", "inner"))),
        out_specs=(rows, rows),
        check_vma=False,
    )
```

```python
import math

import jax
import jax.numpy as jnp
from jax import lax
from jax.experimental import pallas as pl
from jax.experimental.pallas import tpu as pltpu
from jax.sharding import PartitionSpec as P

MESH = pl.DeviceIdType.MESH
F32 = jnp.float32
BF16 = jnp.bfloat16

SCALE = 20.0
EXP2_SCALE = SCALE * math.log2(math.e)
EPSILON = 1e-06
RING = 4
ROWS = 128
HALF = 64
D = 1024
NQ = 2048
NP = 1024

PLACE = {
    (0, 0): 0, (0, 1): 1, (3, 0): 2, (1, 0): 3,
    (3, 1): 4, (1, 1): 5, (2, 0): 6, (2, 1): 7,
}
ORDER = sorted(PLACE, key=PLACE.get)
A, B = 0, 1
SEMAPHORES = 75


def q_row(place, t):
    k = PLACE[place]
    return t * 512 + k * ROWS if k < 4 else k // 2 * 512 + t * 256 + k % 2 * ROWS


class Links:
    def __init__(self, semaphores, device):
        self.semaphores, self.device = semaphores, device
        self.index, self.copies = {}, {}

    def semaphore(self, name):
        i = self.index.setdefault(name, len(self.index))
        assert i < SEMAPHORES
        return self.semaphores.at[i]

    def copy(self, src, dst, sent, landed, device):
        return pltpu.make_async_remote_copy(
            src_ref=src,
            dst_ref=dst,
            send_sem=self.semaphore("sent " + sent),
            recv_sem=self.semaphore("landed " + landed),
            device_id=device,
            device_id_type=MESH,
        )

    def send(self, name, src, dst, device, sent, landed=None):
        copy = self.copy(src, dst, sent, landed or name, device)
        copy.start()
        assert name not in self.copies
        self.copies[name] = copy

    def arrived(self, name):
        self.copies[name].wait_recv()

    def all_arrived(self, landed, like):
        self.copy(like, like, "c", landed, self.device).wait_recv()

    def all_sent(self, sent, like):
        self.copy(like, like, sent, "c1", self.device).wait_send()


def kernel(
    q_hbm, p_hbm, pos_in, q_out, p_out,
    qf, pf, q_len, p_len, qbuf, pbuf, pos_buf, e_ref, w_ref, racc, cacc,
    row_tx, row_rx, col_tx, col_rx, row_tot, col_tot, qpart, ppart, q_d2d, q_rx, p_rx,
    row_inverse, local_sem, copy_sem,
):
    team, inner = lax.axis_index("team"), lax.axis_index("inner")
    x, c = team // 2, team % 2
    z, y = inner // RING, inner % RING
    bit = y % 2

    def device(x, y, z, c):
        return {"team": x * 2 + c, "inner": z * RING + y}

    def q_device(r, s, t):
        yy = y if s == 0 else y + 1 - 2 * bit
        return device((x + r) % RING, yy, z, c if t == 0 else 1 - c)

    def p_device(r, s):
        return device(x, y if s == 0 else 3 - y, (z + r) % RING, c)

    q_peers = [(r, s, t) for r in range(RING) for s in range(2) for t in range(2)][1:]
    p_peers = [(r, s) for r in range(RING) for s in range(2)][1:]

    def far(peer):
        return -min(peer[0], RING - peer[0]) - sum(peer[1:])


    loads = [
        pltpu.make_async_copy(q_hbm, qf, local_sem.at[0]),
        pltpu.make_async_copy(p_hbm, pf, local_sem.at[1]),
    ]
    for load in loads:
        load.start()
    barrier = pltpu.get_barrier_semaphore()
    neighbours = [q_device(*peer) for peer in ((1, 0, 0), (3, 0, 0), (0, 1, 0), (0, 0, 1))]
    neighbours += [p_device(*peer) for peer in ((1, 0), (3, 0), (0, 1))]
    for neighbour in neighbours:
        pl.semaphore_signal(barrier, inc=1, device_id=neighbour, device_id_type=MESH)

    sibling = q_device(0, 0, 1)
    links = Links(copy_sem, sibling)
    send, arrived = links.send, links.arrived

    def normalize(full, length_ref, rounded):
        v = full[...]
        length = jnp.sqrt(jnp.sum(v * v, axis=1, keepdims=True) + EPSILON)
        unit = v / length
        full[...] = unit
        length_ref[...] = jnp.broadcast_to(length, (ROWS, 128))
        rounded[pl.ds(0, ROWS), :] = unit.astype(BF16)

    loads[0].wait()
    normalize(qf, q_len, qbuf)
    loads[1].wait()
    normalize(pf, p_len, pbuf)
    pos_buf[0] = jnp.broadcast_to(pos_in[...], (8, 128))
    racc[...] = jnp.zeros_like(racc)
    cacc[...] = jnp.zeros_like(cacc)
    pl.semaphore_wait(barrier, len(neighbours))

    def q_at(place, half, t=0):
        return qbuf.at[pl.ds(q_row(place, t) + half * HALF, HALF), :]

    def p_at(place, half):
        return pbuf.at[pl.ds(PLACE[place] * ROWS + half * HALF, HALF), :]

    class Gather:
        def __init__(self, tag, at, right, left, pair, on_arrival):
            self.tag, self.at, self.on_arrival = tag, at, on_arrival
            self.to = {"x": right, "l": left, "y": pair}
            self.landed = {}

        def send(self, name, src, dst, half):
            self.landed[name] = (dst, half)
            send(self.tag + name, self.at(src, half), self.at(dst, half), self.to[name[0]], self.tag)

        def take(self, name):
            arrived(self.tag + name)
            self.on_arrival(name, *self.landed[name])

        def begin(self):
            self.send("xA", (0, 0), (3, 0), A)
            self.send("lA", (0, 0), (1, 0), A)
            self.send("yB", (0, 0), (0, 1), B)
            self.send("xB", (0, 0), (3, 0), B)
            self.send("lB", (0, 0), (1, 0), B)
            self.send("yA", (0, 0), (0, 1), A)

        def first(self):
            self.take("xA")
            self.send("xA2", (3, 0), (2, 0), A)
            self.send("yA3", (3, 0), (3, 1), A)
            self.take("lA")
            self.send("yA1", (1, 0), (1, 1), A)
            self.take("yB")
            self.send("xPB", (0, 1), (3, 1), B)
            self.send("lPB", (0, 1), (1, 1), B)

        def second(self):
            self.take("xB")
            self.send("xB2", (3, 0), (2, 0), B)
            self.take("lB")
            self.take("yA")

        def third(self):
            self.take("lPB")
            self.send("lPB2", (1, 1), (2, 1), B)
            self.take("xA2")
            self.send("yA2", (2, 0), (2, 1), A)
            self.take("yA3")

        def fourth(self):
            self.take("xPB")
            self.take("yA1")
            self.take("lPB2")

        def fifth(self):
            self.take("xB2")
            self.take("yA2")

    def share(name, place, half):
        stage = "c1" if PLACE[place] < 4 else "c2" if PLACE[place] < 6 else "c3"
        send("c" + name, q_at(place, half, 0), q_at(place, half, 1), sibling, "c", stage)

    qg = Gather("q", q_at, q_device(1, 0, 0), q_device(3, 0, 0), q_device(0, 1, 0), share)
    pg = Gather("p", p_at, p_device(1, 0), p_device(3, 0), p_device(0, 1), lambda *_: None)
    qg.begin()
    pg.begin()
    send("c", qbuf.at[pl.ds(0, ROWS), :], qbuf.at[pl.ds(512, ROWS), :], sibling, "c", "c1")

    def scores(rows0, rows1, cols0, cols1):
        step = width = 256
        for i in range(rows0, rows1, step):
            rows = pl.ds(i, step)
            for j in range(cols0, cols1, width):
                cols = pl.ds(j, width)
                s = lax.dot_general(
                    qbuf[rows, :],
                    pbuf[cols, :],
                    (((1,), (1,)), ((), ())),
                    preferred_element_type=F32,
                )
                e = jnp.exp2(s * EXP2_SCALE)
                e_ref[rows, cols] = e
                part = e[:, 0:128]
                for k in range(128, width, 128):
                    part = part + e[:, k : k + 128]
                racc[rows, :] += part
                cacc[:, cols] += jnp.sum(e.reshape(step // 8, 8, width), axis=0)

    def landed(stage, rows, count):
        links.all_arrived(stage, qbuf.at[pl.ds(rows, count), :])

    for g in (qg, pg):
        g.first()
    for g in (qg, pg):
        g.second()
    scores(0, 512, 0, 512)
    landed("c1", 512, 512)
    for g in (qg, pg):
        g.third()
    scores(512, 1024, 0, 512)
    for g in (qg, pg):
        g.fourth()
    scores(0, 1024, 512, 768)
    scores(1024, 1280, 0, 768)
    landed("c2", 1280, 256)
    scores(1280, 1536, 0, 768)
    for g in (qg, pg):
        g.fifth()
    blocks = [(place, t) for place in ORDER for t in range(2)]
    for r, s, t in q_peers:
        slot = q_row((-r % RING, s), t) // ROWS
        send(f"pos{r}{s}{t}", pos_buf.at[0], pos_buf.at[slot], q_device(r, s, t), "pos", "pos")
    scores(0, 1536, 768, 1024)
    scores(1536, 1792, 0, 1024)
    landed("c3", 1792, 256)
    scores(1792, 2048, 0, 1024)

    def q_index(r, s, t):
        yb = bit if s == 0 else 1 - bit
        return ((x + r) % RING) * 4 + yb * 2 + (c if t == 0 else 1 - c)

    def p_index(r, s):
        yb = bit if s == 0 else 1 - bit
        return ((z + r) % RING) * 2 + yb

    for k, place in enumerate(ORDER):
        col = jnp.sum(cacc[:, pl.ds(k * ROWS, ROWS)], axis=0, keepdims=True)
        col_tx[pl.ds(p_index(*place), 1), :] = col
    for r, s in sorted(p_peers, key=far):
        slot = (-r % RING) * 2 + s
        send(f"col{r}{s}", col_tx, col_rx.at[slot], p_device(r, s), "col", "col")
    for place, t in blocks:
        turned = jnp.transpose(racc[pl.ds(q_row(place, t), ROWS), :])
        row_tx[pl.ds(q_index(*place, t), 1), :] = jnp.sum(turned, axis=0, keepdims=True)
    for r, s, t in sorted(q_peers, key=far):
        slot = (-r % RING) * 4 + s * 2 + t
        send(f"row{r}{s}{t}", row_tx, row_rx.at[slot], q_device(r, s, t), "row", "row")

    def column_base(place):
        r, s = place
        zz, yy = (z + r) % RING, y if s == 0 else 3 - y
        return (team * 16 + zz * RING + yy) * ROWS

    bases = [column_base(place).astype(F32) for place in ORDER]

    links.all_arrived("pos", pos_buf.at[pl.ds(1, 15)])
    lane = lax.broadcasted_iota(jnp.int32, (ROWS, 128), 1).astype(F32)
    for k in range(16):
        target = jnp.broadcast_to(pos_buf[k, pl.ds(0, 1), :].astype(F32), (128, 128))
        shifted = jnp.transpose(target) - lane
        for j in range(8):
            hit = jnp.where(shifted == bases[j], -2.0, 0.0)
            w_ref[pl.ds(k * ROWS, ROWS), pl.ds(j * 128, 128)] = hit.astype(BF16)
    links.all_arrived("col", col_rx.at[pl.ds(1, 7)])
    total = col_tx[...]
    for i in range(1, 8):
        total = total + col_rx[i]
    col_inverse = 1.0 / total
    col_tot[pl.ds(0, 8), :] = col_inverse
    links.all_arrived("row", row_rx.at[pl.ds(1, 15)])
    total = row_tx[...]
    for i in range(1, 16):
        total = total + row_rx[i]
    row_tot[pl.ds(0, 16), :] = 1.0 / total
    for place, t in blocks:
        row_tot[pl.ds(16 + q_row(place, t) // ROWS, 1), :] = row_tot[pl.ds(q_index(*place, t), 1), :]
    for k, place in enumerate(ORDER):
        col_tot[pl.ds(8 + k, 1), :] = col_tot[pl.ds(p_index(*place), 1), :]

    def row_factor(k):
        rows = pl.ds(k * ROWS, ROWS)
        factor = jnp.broadcast_to(row_tot[pl.ds(16 + k, 1), :], (128, 128))
        row_inverse[rows, :] = jnp.transpose(factor)

    def weight(k, columns):
        rows = pl.ds(k * ROWS, ROWS)
        factor = row_inverse[rows, :]
        for j in columns:
            cols = pl.ds(j * 128, 128)
            w = e_ref[rows, cols] * (factor + col_tot[pl.ds(8 + j, 1), :])
            w_ref[rows, cols] += w.astype(BF16)

    def weights(slots, columns):
        return [(weight, k, columns) for k in slots]

    def run(work):
        for f, *args in work:
            f(*args)

    def q_dot(first, last, beside=()):
        rows = pl.ds(first, last - first)
        for i in range(4):
            cols = pl.ds(i * 256, 256)
            qpart[rows, cols] = jnp.dot(
                w_ref[rows, :], pbuf[:, cols], preferred_element_type=F32
            ).astype(BF16)
            run(beside[len(beside) * i // 4 : len(beside) * (i + 1) // 4])

    def to_sibling(first, rows, place_row):
        send(
            f"d{place_row}",
            qpart.at[pl.ds(first, rows), :],
            q_d2d.at[pl.ds(place_row, rows), :],
            sibling,
            "d",
        )

    def p_dot(first, last, beside=()):
        out = pl.ds(first, last - first)
        for i in range(4):
            cols = pl.ds(i * 256, 256)
            ppart[out, cols] = lax.dot_general(
                w_ref[:, out],
                qbuf[:, cols],
                (((0,), (0,)), ((), ())),
                preferred_element_type=F32,
            ).astype(BF16)
            run(beside[len(beside) * i // 4 : len(beside) * (i + 1) // 4])

    class Reduce:
        def __init__(self, tag, part, row, extra, rx, right, left, pair):
            self.tag, self.part, self.row, self.extra, self.rx = tag, part, row, extra, rx
            self.to = {"x": right, "l": left, "y": pair}
            self.slots = {}

        def rows(self, place, half):
            return pl.ds(self.row(place) + half * HALF, HALF)

        def total(self, place, half, names):
            value = self.part[self.rows(place, half), :].astype(F32)
            if self.extra is not None:
                rows = pl.ds(PLACE[place] * ROWS + half * HALF, HALF)
                value += self.extra[rows, :].astype(F32)
            for name in names:
                arrived(self.tag + name)
                value += self.rx[self.slots[name]].astype(F32)
            return value

        def send(self, name, place, half, *names):
            if names or self.extra is not None:
                self.part[self.rows(place, half), :] = self.total(place, half, names).astype(BF16)
            self.slots[name] = slot = len(self.slots)
            src = self.part.at[self.rows(place, half), :]
            send(self.tag + name, src, self.rx.at[slot], self.to[name[0]], self.tag)

        def one(self):
            self.send("xB0o", (2, 0), B)
            self.send("lB1o", (2, 1), B)
            self.send("yA2", (2, 1), A)

        def two(self):
            self.send("xB1r", (1, 1), B)
            self.send("yA1", (1, 1), A)
            self.send("yA3", (3, 1), A)

        def three(self):
            self.send("lB1l", (3, 1), B, "lB1o")
            self.send("xAo", (2, 0), A, "yA2")

        def four(self):
            self.send("lB0l", (3, 0), B)
            self.send("xB0r", (1, 0), B, "xB0o")
            self.send("yA0", (0, 1), A)

        def five(self):
            self.send("yB1f", (0, 1), B, "xB1r", "lB1l")

        def six(self):
            self.send("lAl", (3, 0), A, "yA3")
            self.send("xAr", (1, 0), A, "yA1", "xAo")

        def finish(self, unit_ref, length_ref, out_ref):
            for half, names in ((B, ("xB0r", "lB0l", "yB1f")), (A, ("yA0", "lAl", "xAr"))):
                rows = pl.ds(half * HALF, HALF)
                raw = self.total((0, 0), half, names) * SCALE
                unit = unit_ref[rows, :]
                along = jnp.sum(unit * raw, axis=1, keepdims=True)
                out_ref[rows, :] = (raw - unit * along) / length_ref[rows, 0:1]

    qr = Reduce(
        "Q", qpart, lambda place: q_row(place, 0), q_d2d, q_rx,
        q_device(1, 0, 0), q_device(3, 0, 0), q_device(0, 1, 0),
    )
    pr = Reduce(
        "P", ppart, lambda place: PLACE[place] * ROWS, None, p_rx,
        p_device(1, 0), p_device(3, 0), p_device(0, 1),
    )

    for k in range(12, 16):
        row_factor(k)
    run(weights(range(12, 16), range(8)))
    later = [(row_factor, k) for k in range(12)] + weights(range(12), (6, 7))
    q_dot(1792, 2048, later)
    to_sibling(1792, 256, 768)
    p_dot(768, 1024, weights(range(12), (4, 5)))
    pr.one()
    q_dot(1536, 1792, weights(range(8, 12), range(4)))
    arrived("d768")
    qr.one()
    later = weights(range(8), range(4))
    q_dot(1280, 1536, later[:2])
    to_sibling(1280, 256, 512)
    p_dot(512, 768, later[2:6])
    pr.two()
    q_dot(1024, 1280, later[6:])
    arrived("d512")
    qr.two()
    p_dot(128, 512)
    pr.three()
    pr.four()
    qr.three()
    q_dot(640, 1024)
    to_sibling(640, 384, 128)
    q_dot(128, 512)
    q_dot(512, 640)
    to_sibling(512, 128, 0)
    q_dot(0, 128)
    arrived("d128")
    qr.four()
    pr.five()
    p_dot(0, 128)
    pr.six()
    qr.five()
    qr.six()
    arrived("d0")
    pr.finish(pf, p_len, p_out)
    qr.finish(qf, q_len, q_out)
    for sent, like in (
        ("q", q_rx), ("p", p_rx), ("Q", q_rx), ("P", p_rx),
        ("c", q_d2d), ("d", q_d2d),
        ("pos", pos_buf.at[pl.ds(1, 15)]),
        ("row", row_rx.at[pl.ds(1, 15)]),
        ("col", col_rx.at[pl.ds(1, 7)]),
    ):
        links.all_sent(sent, like)


def put_out(q_in, p_in, q_hbm, p_hbm, sem):
    copies = [
        pltpu.make_async_copy(q_in, q_hbm, sem.at[0]),
        pltpu.make_async_copy(p_in, p_hbm, sem.at[1]),
    ]
    for copy in copies:
        copy.start()
    for copy in copies:
        copy.wait()


def per_device(queries, passages, positive):
    vmem = pltpu.VMEM
    scratch = [
        vmem((ROWS, D), F32),
        vmem((ROWS, D), F32),
        vmem((ROWS, 128), F32),
        vmem((ROWS, 128), F32),
        vmem((NQ, D), BF16),
        vmem((NP, D), BF16),
        vmem((16, 8, 128), jnp.int32),
        vmem((NQ, NP), F32),
        vmem((NQ, NP), BF16),
        vmem((NQ, 128), F32),
        vmem((8, NP), F32),
        vmem((16, 128), F32),
        vmem((16, 16, 128), F32),
        vmem((8, 128), F32),
        vmem((8, 8, 128), F32),
        vmem((32, 128), F32),
        vmem((16, 128), F32),
        vmem((NQ, D), BF16),
        vmem((NP, D), BF16),
        vmem((1024, D), BF16),
        vmem((14, HALF, D), BF16),
        vmem((14, HALF, D), BF16),
        vmem((NQ, 128), F32),
        pltpu.SemaphoreType.DMA((2,)),
        pltpu.SemaphoreType.DMA((SEMAPHORES,)),
    ]
    out = jax.ShapeDtypeStruct((ROWS, D), F32)
    here = pl.BlockSpec(memory_space=pltpu.VMEM)
    hbm = pl.BlockSpec(memory_space=pltpu.HBM)
    grads = pl.pallas_call(
        kernel,
        out_shape=(out, out),
        in_specs=[hbm, hbm, here],
        out_specs=(here, here),
        scratch_shapes=scratch,
        compiler_params=pltpu.CompilerParams(
            collective_id=0, has_side_effects=True, vmem_limit_bytes=52 << 20
        ),
    )(queries, passages, positive.reshape(1, ROWS))
    return pl.pallas_call(
        put_out,
        out_shape=(out, out),
        in_specs=[here, here],
        out_specs=(hbm, hbm),
        scratch_shapes=[pltpu.SemaphoreType.DMA((2,))],
        compiler_params=pltpu.CompilerParams(vmem_limit_bytes=1 << 20),
    )(*grads)


def solution(mesh):
    rows = P(("team", "inner"), None)
    return jax.shard_map(
        per_device,
        mesh=mesh,
        in_specs=(rows, rows, P(("team", "inner"))),
        out_specs=(rows, rows),
        check_vma=False,
    )
```

```python
import math

import jax
import jax.numpy as jnp
from jax import lax
from jax.experimental import pallas as pl
from jax.experimental.pallas import tpu as pltpu
from jax.sharding import PartitionSpec as P

MESH = pl.DeviceIdType.MESH
F32 = jnp.float32
BF16 = jnp.bfloat16

SCALE = 20.0
EXP2_SCALE = SCALE * math.log2(math.e)
EPSILON = 1e-06
RING = 4
ROWS = 128
HALF = 64
D = 1024
NQ = 2048
NP = 1024

PLACE = {
    (0, 0): 0, (0, 1): 1, (3, 0): 2, (1, 0): 3,
    (3, 1): 4, (1, 1): 5, (2, 0): 6, (2, 1): 7,
}
ORDER = sorted(PLACE, key=PLACE.get)
A, B = 0, 1
SEMAPHORES = 75


def q_row(place, t):
    k = PLACE[place]
    return t * 512 + k * ROWS if k < 4 else k // 2 * 512 + t * 256 + k % 2 * ROWS


class Links:
    def __init__(self, semaphores, device):
        self.semaphores, self.device = semaphores, device
        self.index, self.copies = {}, {}

    def semaphore(self, name):
        i = self.index.setdefault(name, len(self.index))
        assert i < SEMAPHORES
        return self.semaphores.at[i]

    def copy(self, src, dst, sent, landed, device):
        return pltpu.make_async_remote_copy(
            src_ref=src,
            dst_ref=dst,
            send_sem=self.semaphore("sent " + sent),
            recv_sem=self.semaphore("landed " + landed),
            device_id=device,
            device_id_type=MESH,
        )

    def send(self, name, src, dst, device, sent, landed=None):
        copy = self.copy(src, dst, sent, landed or name, device)
        copy.start()
        assert name not in self.copies
        self.copies[name] = copy

    def arrived(self, name):
        self.copies[name].wait_recv()

    def all_arrived(self, landed, like):
        self.copy(like, like, "c", landed, self.device).wait_recv()

    def all_sent(self, sent, like):
        self.copy(like, like, sent, "c1", self.device).wait_send()


def kernel(
    q_hbm, p_hbm, pos_in, q_out, p_out,
    qf, pf, q_len, p_len, qbuf, pbuf, pos_buf, e_ref, w_ref, racc, cacc,
    row_tx, row_rx, col_tx, col_rx, row_tot, col_tot, qpart, ppart, q_d2d, q_rx, p_rx,
    row_inverse, local_sem, copy_sem,
):
    team, inner = lax.axis_index("team"), lax.axis_index("inner")
    x, c = team // 2, team % 2
    z, y = inner // RING, inner % RING
    bit = y % 2

    def device(x, y, z, c):
        return {"team": x * 2 + c, "inner": z * RING + y}

    def q_device(r, s, t):
        yy = y if s == 0 else y + 1 - 2 * bit
        return device((x + r) % RING, yy, z, c if t == 0 else 1 - c)

    def p_device(r, s):
        return device(x, y if s == 0 else 3 - y, (z + r) % RING, c)

    q_peers = [(r, s, t) for r in range(RING) for s in range(2) for t in range(2)][1:]
    p_peers = [(r, s) for r in range(RING) for s in range(2)][1:]

    def far(peer):
        return -min(peer[0], RING - peer[0]) - sum(peer[1:])


    loads = [
        pltpu.make_async_copy(q_hbm, qf, local_sem.at[0]),
        pltpu.make_async_copy(p_hbm, pf, local_sem.at[1]),
    ]
    for load in loads:
        load.start()
    barrier = pltpu.get_barrier_semaphore()
    neighbours = [q_device(*peer) for peer in ((1, 0, 0), (3, 0, 0), (0, 1, 0), (0, 0, 1))]
    neighbours += [p_device(*peer) for peer in ((1, 0), (3, 0), (0, 1))]
    for neighbour in neighbours:
        pl.semaphore_signal(barrier, inc=1, device_id=neighbour, device_id_type=MESH)

    sibling = q_device(0, 0, 1)
    links = Links(copy_sem, sibling)
    send, arrived = links.send, links.arrived

    def normalize(full, length_ref, rounded):
        v = full[...]
        length = jnp.sqrt(jnp.sum(v * v, axis=1, keepdims=True) + EPSILON)
        unit = v / length
        full[...] = unit
        length_ref[...] = jnp.broadcast_to(length, (ROWS, 128))
        rounded[pl.ds(0, ROWS), :] = unit.astype(BF16)

    loads[0].wait()
    normalize(qf, q_len, qbuf)
    loads[1].wait()
    normalize(pf, p_len, pbuf)
    pos_buf[0] = jnp.broadcast_to(pos_in[...], (8, 128))
    racc[...] = jnp.zeros_like(racc)
    cacc[...] = jnp.zeros_like(cacc)
    pl.semaphore_wait(barrier, len(neighbours))

    def q_at(place, half, t=0):
        return qbuf.at[pl.ds(q_row(place, t) + half * HALF, HALF), :]

    def p_at(place, half):
        return pbuf.at[pl.ds(PLACE[place] * ROWS + half * HALF, HALF), :]

    class Gather:
        def __init__(self, tag, at, right, left, pair, on_arrival):
            self.tag, self.at, self.on_arrival = tag, at, on_arrival
            self.to = {"x": right, "l": left, "y": pair}
            self.landed = {}

        def send(self, name, src, dst, half):
            self.landed[name] = (dst, half)
            send(self.tag + name, self.at(src, half), self.at(dst, half), self.to[name[0]], self.tag)

        def take(self, name):
            arrived(self.tag + name)
            self.on_arrival(name, *self.landed[name])

        def begin(self):
            self.send("xA", (0, 0), (3, 0), A)
            self.send("lA", (0, 0), (1, 0), A)
            self.send("yB", (0, 0), (0, 1), B)
            self.send("xB", (0, 0), (3, 0), B)
            self.send("lB", (0, 0), (1, 0), B)
            self.send("yA", (0, 0), (0, 1), A)

        def first(self):
            self.take("xA")
            self.send("xA2", (3, 0), (2, 0), A)
            self.send("yA3", (3, 0), (3, 1), A)
            self.take("lA")
            self.send("yA1", (1, 0), (1, 1), A)
            self.take("yB")
            self.send("xPB", (0, 1), (3, 1), B)
            self.send("lPB", (0, 1), (1, 1), B)

        def second(self):
            self.take("xB")
            self.send("xB2", (3, 0), (2, 0), B)
            self.take("lB")
            self.take("yA")

        def third(self):
            self.take("lPB")
            self.send("lPB2", (1, 1), (2, 1), B)
            self.take("xA2")
            self.send("yA2", (2, 0), (2, 1), A)
            self.take("yA3")

        def fourth(self):
            self.take("xPB")
            self.take("yA1")

        def fifth(self):
            self.take("xB2")
            self.take("yA2")

    def share(name, place, half):
        stage = "c1" if PLACE[place] < 4 else "c2" if PLACE[place] < 6 else "c3"
        send("c" + name, q_at(place, half, 0), q_at(place, half, 1), sibling, "c", stage)

    qg = Gather("q", q_at, q_device(1, 0, 0), q_device(3, 0, 0), q_device(0, 1, 0), share)
    pg = Gather("p", p_at, p_device(1, 0), p_device(3, 0), p_device(0, 1), lambda *_: None)
    qg.begin()
    pg.begin()
    send("c", qbuf.at[pl.ds(0, ROWS), :], qbuf.at[pl.ds(512, ROWS), :], sibling, "c", "c1")

    def scores(rows0, rows1, cols0, cols1):
        step = width = 256
        for i in range(rows0, rows1, step):
            rows = pl.ds(i, step)
            for j in range(cols0, cols1, width):
                cols = pl.ds(j, width)
                s = lax.dot_general(
                    qbuf[rows, :],
                    pbuf[cols, :],
                    (((1,), (1,)), ((), ())),
                    preferred_element_type=F32,
                )
                e = jnp.exp2(s * EXP2_SCALE)
                e_ref[rows, cols] = e
                part = e[:, 0:128]
                for k in range(128, width, 128):
                    part = part + e[:, k : k + 128]
                racc[rows, :] += part
                cacc[:, cols] += jnp.sum(e.reshape(step // 8, 8, width), axis=0)

    def q_index(r, s, t):
        yb = bit if s == 0 else 1 - bit
        return ((x + r) % RING) * 4 + yb * 2 + (c if t == 0 else 1 - c)

    def sum_rows(blocks):
        for place, t in blocks:
            turned = jnp.transpose(racc[pl.ds(q_row(place, t), ROWS), :])
            row_tx[pl.ds(q_index(*place, t), 1), :] = jnp.sum(turned, axis=0, keepdims=True)

    def landed(stage, rows, count):
        links.all_arrived(stage, qbuf.at[pl.ds(rows, count), :])

    for g in (qg, pg):
        g.first()
    for g in (qg, pg):
        g.second()
    scores(0, 512, 0, 512)
    landed("c1", 512, 512)
    for g in (qg, pg):
        g.third()
    scores(512, 1024, 0, 512)
    for g in (qg, pg):
        g.fourth()
    scores(0, 1024, 512, 768)
    scores(1024, 1280, 0, 768)
    for g in (qg, pg):
        g.take("lPB2")
    landed("c2", 1280, 256)
    scores(1280, 1536, 0, 768)
    for g in (qg, pg):
        g.fifth()
    blocks = sorted(((place, t) for place in ORDER for t in range(2)), key=lambda b: q_row(*b))
    for r, s, t in q_peers:
        slot = q_row((-r % RING, s), t) // ROWS
        send(f"pos{r}{s}{t}", pos_buf.at[0], pos_buf.at[slot], q_device(r, s, t), "pos", "pos")
    scores(0, 1536, 768, 1024)
    scores(1536, 1792, 0, 1024)
    sum_rows(blocks[:-2])
    landed("c3", 1792, 256)
    scores(1792, 2048, 0, 1024)

    def p_index(r, s):
        yb = bit if s == 0 else 1 - bit
        return ((z + r) % RING) * 2 + yb

    for k, place in enumerate(ORDER):
        col = jnp.sum(cacc[:, pl.ds(k * ROWS, ROWS)], axis=0, keepdims=True)
        col_tx[pl.ds(p_index(*place), 1), :] = col
    for r, s in sorted(p_peers, key=far):
        slot = (-r % RING) * 2 + s
        send(f"col{r}{s}", col_tx, col_rx.at[slot], p_device(r, s), "col", "col")
    sum_rows(blocks[-2:])
    for r, s, t in sorted(q_peers, key=far):
        slot = (-r % RING) * 4 + s * 2 + t
        send(f"row{r}{s}{t}", row_tx, row_rx.at[slot], q_device(r, s, t), "row", "row")

    def column_base(place):
        r, s = place
        zz, yy = (z + r) % RING, y if s == 0 else 3 - y
        return (team * 16 + zz * RING + yy) * ROWS

    bases = [column_base(place).astype(F32) for place in ORDER]

    links.all_arrived("pos", pos_buf.at[pl.ds(1, 15)])
    lane = lax.broadcasted_iota(jnp.int32, (ROWS, 128), 1).astype(F32)
    for k in range(16):
        target = jnp.broadcast_to(pos_buf[k, pl.ds(0, 1), :].astype(F32), (128, 128))
        shifted = jnp.transpose(target) - lane
        for j in range(8):
            hit = jnp.where(shifted == bases[j], -2.0, 0.0)
            w_ref[pl.ds(k * ROWS, ROWS), pl.ds(j * 128, 128)] = hit.astype(BF16)
    links.all_arrived("col", col_rx.at[pl.ds(1, 7)])
    total = col_tx[...]
    for i in range(1, 8):
        total = total + col_rx[i]
    col_inverse = 1.0 / total
    col_tot[pl.ds(0, 8), :] = col_inverse
    links.all_arrived("row", row_rx.at[pl.ds(1, 15)])
    total = row_tx[...]
    for i in range(1, 16):
        total = total + row_rx[i]
    row_tot[pl.ds(0, 16), :] = 1.0 / total
    for place, t in blocks:
        row_tot[pl.ds(16 + q_row(place, t) // ROWS, 1), :] = row_tot[pl.ds(q_index(*place, t), 1), :]
    for k, place in enumerate(ORDER):
        col_tot[pl.ds(8 + k, 1), :] = col_tot[pl.ds(p_index(*place), 1), :]

    def row_factor(k):
        rows = pl.ds(k * ROWS, ROWS)
        factor = jnp.broadcast_to(row_tot[pl.ds(16 + k, 1), :], (128, 128))
        row_inverse[rows, :] = jnp.transpose(factor)

    def weight(k, columns):
        rows = pl.ds(k * ROWS, ROWS)
        factor = row_inverse[rows, :]
        for j in columns:
            cols = pl.ds(j * 128, 128)
            w = e_ref[rows, cols] * (factor + col_tot[pl.ds(8 + j, 1), :])
            w_ref[rows, cols] += w.astype(BF16)

    def weights(slots, columns):
        return [(weight, k, columns) for k in slots]

    def run(work):
        for f, *args in work:
            f(*args)

    def q_dot(first, last, beside=()):
        rows = pl.ds(first, last - first)
        for i in range(4):
            cols = pl.ds(i * 256, 256)
            qpart[rows, cols] = jnp.dot(
                w_ref[rows, :], pbuf[:, cols], preferred_element_type=F32
            ).astype(BF16)
            run(beside[len(beside) * i // 4 : len(beside) * (i + 1) // 4])

    def to_sibling(first, rows, place_row):
        send(
            f"d{place_row}",
            qpart.at[pl.ds(first, rows), :],
            q_d2d.at[pl.ds(place_row, rows), :],
            sibling,
            "d",
        )

    def p_dot(first, last, beside=()):
        out = pl.ds(first, last - first)
        for i in range(4):
            cols = pl.ds(i * 256, 256)
            ppart[out, cols] = lax.dot_general(
                w_ref[:, out],
                qbuf[:, cols],
                (((0,), (0,)), ((), ())),
                preferred_element_type=F32,
            ).astype(BF16)
            run(beside[len(beside) * i // 4 : len(beside) * (i + 1) // 4])

    class Reduce:
        def __init__(self, tag, part, row, extra, rx, right, left, pair):
            self.tag, self.part, self.row, self.extra, self.rx = tag, part, row, extra, rx
            self.to = {"x": right, "l": left, "y": pair}
            self.slots = {}

        def rows(self, place, half):
            return pl.ds(self.row(place) + half * HALF, HALF)

        def total(self, place, half, names):
            value = self.part[self.rows(place, half), :].astype(F32)
            if self.extra is not None:
                rows = pl.ds(PLACE[place] * ROWS + half * HALF, HALF)
                value += self.extra[rows, :].astype(F32)
            for name in names:
                arrived(self.tag + name)
                value += self.rx[self.slots[name]].astype(F32)
            return value

        def send(self, name, place, half, *names):
            if names or self.extra is not None:
                self.part[self.rows(place, half), :] = self.total(place, half, names).astype(BF16)
            self.slots[name] = slot = len(self.slots)
            src = self.part.at[self.rows(place, half), :]
            send(self.tag + name, src, self.rx.at[slot], self.to[name[0]], self.tag)

        def one(self):
            self.send("xB0o", (2, 0), B)
            self.send("lB1o", (2, 1), B)
            self.send("yA2", (2, 1), A)

        def two(self):
            self.send("xB1r", (1, 1), B)
            self.send("yA1", (1, 1), A)
            self.send("yA3", (3, 1), A)

        def three(self):
            self.send("lB1l", (3, 1), B, "lB1o")
            self.send("xAo", (2, 0), A, "yA2")

        def four(self):
            self.send("lB0l", (3, 0), B)
            self.send("xB0r", (1, 0), B, "xB0o")
            self.send("yA0", (0, 1), A)

        def five(self):
            self.send("yB1f", (0, 1), B, "xB1r", "lB1l")

        def six(self):
            self.send("lAl", (3, 0), A, "yA3")
            self.send("xAr", (1, 0), A, "yA1", "xAo")

        def finish(self, unit_ref, length_ref, out_ref):
            for half, names in ((B, ("xB0r", "lB0l", "yB1f")), (A, ("yA0", "lAl", "xAr"))):
                rows = pl.ds(half * HALF, HALF)
                raw = self.total((0, 0), half, names) * SCALE
                unit = unit_ref[rows, :]
                along = jnp.sum(unit * raw, axis=1, keepdims=True)
                out_ref[rows, :] = (raw - unit * along) / length_ref[rows, 0:1]

    qr = Reduce(
        "Q", qpart, lambda place: q_row(place, 0), q_d2d, q_rx,
        q_device(1, 0, 0), q_device(3, 0, 0), q_device(0, 1, 0),
    )
    pr = Reduce(
        "P", ppart, lambda place: PLACE[place] * ROWS, None, p_rx,
        p_device(1, 0), p_device(3, 0), p_device(0, 1),
    )

    for k in range(12, 16):
        row_factor(k)
    run(weights(range(12, 16), range(8)))
    later = [(row_factor, k) for k in range(12)] + weights(range(12), (6, 7))
    q_dot(1792, 2048, later)
    to_sibling(1792, 256, 768)
    p_dot(768, 1024, weights(range(12), (4, 5)))
    pr.one()
    q_dot(1536, 1792, weights(range(8, 12), range(4)))
    arrived("d768")
    qr.one()
    later = weights(range(8), range(4))
    q_dot(1280, 1536, later[:2])
    to_sibling(1280, 256, 512)
    p_dot(512, 768, later[2:6])
    pr.two()
    q_dot(1024, 1280, later[6:])
    arrived("d512")
    qr.two()
    p_dot(128, 512)
    pr.three()
    pr.four()
    qr.three()
    q_dot(640, 1024)
    to_sibling(640, 384, 128)
    q_dot(128, 512)
    q_dot(512, 640)
    to_sibling(512, 128, 0)
    q_dot(0, 128)
    arrived("d128")
    qr.four()
    pr.five()
    p_dot(0, 128)
    pr.six()
    qr.five()
    qr.six()
    arrived("d0")
    pr.finish(pf, p_len, p_out)
    qr.finish(qf, q_len, q_out)
    for sent, like in (
        ("q", q_rx), ("p", p_rx), ("Q", q_rx), ("P", p_rx),
        ("c", q_d2d), ("d", q_d2d),
        ("pos", pos_buf.at[pl.ds(1, 15)]),
        ("row", row_rx.at[pl.ds(1, 15)]),
        ("col", col_rx.at[pl.ds(1, 7)]),
    ):
        links.all_sent(sent, like)


def put_out(q_in, p_in, q_hbm, p_hbm, sem):
    copies = [
        pltpu.make_async_copy(q_in, q_hbm, sem.at[0]),
        pltpu.make_async_copy(p_in, p_hbm, sem.at[1]),
    ]
    for copy in copies:
        copy.start()
    for copy in copies:
        copy.wait()


def per_device(queries, passages, positive):
    vmem = pltpu.VMEM
    scratch = [
        vmem((ROWS, D), F32),
        vmem((ROWS, D), F32),
        vmem((ROWS, 128), F32),
        vmem((ROWS, 128), F32),
        vmem((NQ, D), BF16),
        vmem((NP, D), BF16),
        vmem((16, 8, 128), jnp.int32),
        vmem((NQ, NP), F32),
        vmem((NQ, NP), BF16),
        vmem((NQ, 128), F32),
        vmem((8, NP), F32),
        vmem((16, 128), F32),
        vmem((16, 16, 128), F32),
        vmem((8, 128), F32),
        vmem((8, 8, 128), F32),
        vmem((32, 128), F32),
        vmem((16, 128), F32),
        vmem((NQ, D), BF16),
        vmem((NP, D), BF16),
        vmem((1024, D), BF16),
        vmem((14, HALF, D), BF16),
        vmem((14, HALF, D), BF16),
        vmem((NQ, 128), F32),
        pltpu.SemaphoreType.DMA((2,)),
        pltpu.SemaphoreType.DMA((SEMAPHORES,)),
    ]
    out = jax.ShapeDtypeStruct((ROWS, D), F32)
    here = pl.BlockSpec(memory_space=pltpu.VMEM)
    hbm = pl.BlockSpec(memory_space=pltpu.HBM)
    grads = pl.pallas_call(
        kernel,
        out_shape=(out, out),
        in_specs=[hbm, hbm, here],
        out_specs=(here, here),
        scratch_shapes=scratch,
        compiler_params=pltpu.CompilerParams(
            collective_id=0, has_side_effects=True, vmem_limit_bytes=52 << 20
        ),
    )(queries, passages, positive.reshape(1, ROWS))
    return pl.pallas_call(
        put_out,
        out_shape=(out, out),
        in_specs=[here, here],
        out_specs=(hbm, hbm),
        scratch_shapes=[pltpu.SemaphoreType.DMA((2,))],
        compiler_params=pltpu.CompilerParams(vmem_limit_bytes=1 << 20),
    )(*grads)


def solution(mesh):
    rows = P(("team", "inner"), None)
    return jax.shard_map(
        per_device,
        mesh=mesh,
        in_specs=(rows, rows, P(("team", "inner"))),
        out_specs=(rows, rows),
        check_vma=False,
    )
```

```python
import math

import jax
import jax.numpy as jnp
from jax import lax
from jax.experimental import pallas as pl
from jax.experimental.pallas import tpu as pltpu
from jax.sharding import PartitionSpec as P

MESH = pl.DeviceIdType.MESH
F32 = jnp.float32
BF16 = jnp.bfloat16

SCALE = 20.0
EXP2_SCALE = SCALE * math.log2(math.e)
EPSILON = 1e-06
RING = 4
ROWS = 128
HALF = 64
D = 1024
NQ = 2048
NP = 1024

PLACE = {
    (0, 0): 0, (0, 1): 1, (3, 0): 2, (1, 0): 3,
    (3, 1): 4, (1, 1): 5, (2, 0): 6, (2, 1): 7,
}
ORDER = sorted(PLACE, key=PLACE.get)
A, B = 0, 1
SEMAPHORES = 75


def q_row(place, t):
    k = PLACE[place]
    return t * 512 + k * ROWS if k < 4 else k // 2 * 512 + t * 256 + k % 2 * ROWS


class Links:
    def __init__(self, semaphores, device):
        self.semaphores, self.device = semaphores, device
        self.index, self.copies = {}, {}

    def semaphore(self, name):
        i = self.index.setdefault(name, len(self.index))
        assert i < SEMAPHORES
        return self.semaphores.at[i]

    def copy(self, src, dst, sent, landed, device):
        return pltpu.make_async_remote_copy(
            src_ref=src,
            dst_ref=dst,
            send_sem=self.semaphore("sent " + sent),
            recv_sem=self.semaphore("landed " + landed),
            device_id=device,
            device_id_type=MESH,
        )

    def send(self, name, src, dst, device, sent, landed=None):
        copy = self.copy(src, dst, sent, landed or name, device)
        copy.start()
        assert name not in self.copies
        self.copies[name] = copy

    def arrived(self, name):
        self.copies[name].wait_recv()

    def all_arrived(self, landed, like):
        self.copy(like, like, "c", landed, self.device).wait_recv()

    def all_sent(self, sent, like):
        self.copy(like, like, sent, "c1", self.device).wait_send()


def kernel(
    q_hbm, p_hbm, pos_hbm, q_out, p_out,
    qf, pf, pos_in, q_len, p_len, qbuf, pbuf, pos_buf, e_ref, w_ref, racc, cacc,
    row_tx, row_rx, col_tx, col_rx, row_tot, col_tot, qpart, ppart, q_d2d, q_rx, p_rx,
    row_inverse, local_sem, copy_sem,
):
    team, inner = lax.axis_index("team"), lax.axis_index("inner")
    x, c = team // 2, team % 2
    z, y = inner // RING, inner % RING
    bit = y % 2

    def device(x, y, z, c):
        return {"team": x * 2 + c, "inner": z * RING + y}

    def q_device(r, s, t):
        yy = y if s == 0 else y + 1 - 2 * bit
        return device((x + r) % RING, yy, z, c if t == 0 else 1 - c)

    def p_device(r, s):
        return device(x, y if s == 0 else 3 - y, (z + r) % RING, c)

    q_peers = [(r, s, t) for r in range(RING) for s in range(2) for t in range(2)][1:]
    p_peers = [(r, s) for r in range(RING) for s in range(2)][1:]

    def far(peer):
        return -min(peer[0], RING - peer[0]) - sum(peer[1:])


    loads = [
        pltpu.make_async_copy(q_hbm, qf, local_sem.at[0]),
        pltpu.make_async_copy(p_hbm, pf, local_sem.at[1]),
        pltpu.make_async_copy(pos_hbm, pos_in, local_sem.at[2]),
    ]
    for load in loads:
        load.start()
    barrier = pltpu.get_barrier_semaphore()
    neighbours = [q_device(*peer) for peer in ((1, 0, 0), (3, 0, 0), (0, 1, 0), (0, 0, 1))]
    neighbours += [p_device(*peer) for peer in ((1, 0), (3, 0), (0, 1))]
    for neighbour in neighbours:
        pl.semaphore_signal(barrier, inc=1, device_id=neighbour, device_id_type=MESH)

    sibling = q_device(0, 0, 1)
    links = Links(copy_sem, sibling)
    send, arrived = links.send, links.arrived

    def normalize(full, length_ref, rounded):
        v = full[...]
        length = jnp.sqrt(jnp.sum(v * v, axis=1, keepdims=True) + EPSILON)
        unit = v / length
        full[...] = unit
        length_ref[...] = jnp.broadcast_to(length, (ROWS, 128))
        rounded[pl.ds(0, ROWS), :] = unit.astype(BF16)

    loads[0].wait()
    normalize(qf, q_len, qbuf)
    loads[1].wait()
    normalize(pf, p_len, pbuf)
    pl.semaphore_wait(barrier, len(neighbours))

    def q_at(place, half, t=0):
        return qbuf.at[pl.ds(q_row(place, t) + half * HALF, HALF), :]

    def p_at(place, half):
        return pbuf.at[pl.ds(PLACE[place] * ROWS + half * HALF, HALF), :]

    class Gather:
        def __init__(self, tag, at, right, left, pair, on_arrival):
            self.tag, self.at, self.on_arrival = tag, at, on_arrival
            self.to = {"x": right, "l": left, "y": pair}
            self.landed = {}

        def send(self, name, src, dst, half):
            self.landed[name] = (dst, half)
            send(self.tag + name, self.at(src, half), self.at(dst, half), self.to[name[0]], self.tag)

        def take(self, name):
            arrived(self.tag + name)
            self.on_arrival(name, *self.landed[name])

        def begin(self):
            self.send("xA", (0, 0), (3, 0), A)
            self.send("lA", (0, 0), (1, 0), A)
            self.send("yB", (0, 0), (0, 1), B)
            self.send("xB", (0, 0), (3, 0), B)
            self.send("lB", (0, 0), (1, 0), B)
            self.send("yA", (0, 0), (0, 1), A)

        def first(self):
            self.take("xA")
            self.send("xA2", (3, 0), (2, 0), A)
            self.send("yA3", (3, 0), (3, 1), A)
            self.take("lA")
            self.send("yA1", (1, 0), (1, 1), A)
            self.take("yB")
            self.send("xPB", (0, 1), (3, 1), B)
            self.send("lPB", (0, 1), (1, 1), B)

        def second(self):
            self.take("xB")
            self.send("xB2", (3, 0), (2, 0), B)
            self.take("lB")
            self.take("yA")

        def third(self):
            self.take("lPB")
            self.send("lPB2", (1, 1), (2, 1), B)
            self.take("xA2")
            self.send("yA2", (2, 0), (2, 1), A)
            self.take("yA3")

        def fourth(self):
            self.take("xPB")
            self.take("yA1")

        def fifth(self):
            self.take("xB2")
            self.take("yA2")

    def share(name, place, half):
        stage = "c1" if PLACE[place] < 4 else "c2" if PLACE[place] < 6 else "c3"
        send("c" + name, q_at(place, half, 0), q_at(place, half, 1), sibling, "c", stage)

    qg = Gather("q", q_at, q_device(1, 0, 0), q_device(3, 0, 0), q_device(0, 1, 0), share)
    pg = Gather("p", p_at, p_device(1, 0), p_device(3, 0), p_device(0, 1), lambda *_: None)
    qg.begin()
    pg.begin()
    send("c", qbuf.at[pl.ds(0, ROWS), :], qbuf.at[pl.ds(512, ROWS), :], sibling, "c", "c1")
    loads[2].wait()
    pos_buf[0] = jnp.broadcast_to(pos_in[...], (8, 128))
    racc[...] = jnp.zeros_like(racc)
    cacc[...] = jnp.zeros_like(cacc)

    def scores(rows0, rows1, cols0, cols1):
        step = width = 256
        for i in range(rows0, rows1, step):
            rows = pl.ds(i, step)
            for j in range(cols0, cols1, width):
                cols = pl.ds(j, width)
                s = lax.dot_general(
                    qbuf[rows, :],
                    pbuf[cols, :],
                    (((1,), (1,)), ((), ())),
                    preferred_element_type=F32,
                )
                e = jnp.exp2(s * EXP2_SCALE)
                e_ref[rows, cols] = e
                part = e[:, 0:128]
                for k in range(128, width, 128):
                    part = part + e[:, k : k + 128]
                racc[rows, :] += part
                cacc[:, cols] += jnp.sum(e.reshape(step // 8, 8, width), axis=0)

    def q_index(r, s, t):
        yb = bit if s == 0 else 1 - bit
        return ((x + r) % RING) * 4 + yb * 2 + (c if t == 0 else 1 - c)

    def sum_rows(blocks):
        for place, t in blocks:
            turned = jnp.transpose(racc[pl.ds(q_row(place, t), ROWS), :])
            row_tx[pl.ds(q_index(*place, t), 1), :] = jnp.sum(turned, axis=0, keepdims=True)

    def landed(stage, rows, count):
        links.all_arrived(stage, qbuf.at[pl.ds(rows, count), :])

    for g in (qg, pg):
        g.first()
    for g in (qg, pg):
        g.second()
    scores(0, 512, 0, 512)
    landed("c1", 512, 512)
    for g in (qg, pg):
        g.third()
    scores(512, 1024, 0, 512)
    for g in (qg, pg):
        g.fourth()
    scores(0, 1024, 512, 768)
    scores(1024, 1280, 0, 768)
    for g in (qg, pg):
        g.take("lPB2")
    landed("c2", 1280, 256)
    scores(1280, 1536, 0, 768)
    for g in (qg, pg):
        g.fifth()
    blocks = sorted(((place, t) for place in ORDER for t in range(2)), key=lambda b: q_row(*b))
    for r, s, t in q_peers:
        slot = q_row((-r % RING, s), t) // ROWS
        send(f"pos{r}{s}{t}", pos_buf.at[0], pos_buf.at[slot], q_device(r, s, t), "pos", "pos")
    scores(0, 1536, 768, 1024)
    scores(1536, 1792, 0, 1024)
    sum_rows(blocks[:-2])
    landed("c3", 1792, 256)
    scores(1792, 2048, 0, 1024)

    def p_index(r, s):
        yb = bit if s == 0 else 1 - bit
        return ((z + r) % RING) * 2 + yb

    for k, place in enumerate(ORDER):
        col = jnp.sum(cacc[:, pl.ds(k * ROWS, ROWS)], axis=0, keepdims=True)
        col_tx[pl.ds(p_index(*place), 1), :] = col
    for r, s in sorted(p_peers, key=far):
        slot = (-r % RING) * 2 + s
        send(f"col{r}{s}", col_tx, col_rx.at[slot], p_device(r, s), "col", "col")
    sum_rows(blocks[-2:])
    for r, s, t in sorted(q_peers, key=far):
        slot = (-r % RING) * 4 + s * 2 + t
        send(f"row{r}{s}{t}", row_tx, row_rx.at[slot], q_device(r, s, t), "row", "row")

    def column_base(place):
        r, s = place
        zz, yy = (z + r) % RING, y if s == 0 else 3 - y
        return (team * 16 + zz * RING + yy) * ROWS

    bases = [column_base(place).astype(F32) for place in ORDER]

    links.all_arrived("pos", pos_buf.at[pl.ds(1, 15)])
    lane = lax.broadcasted_iota(jnp.int32, (ROWS, 128), 1).astype(F32)
    for k in range(16):
        target = jnp.broadcast_to(pos_buf[k, pl.ds(0, 1), :].astype(F32), (128, 128))
        shifted = jnp.transpose(target) - lane
        for j in range(8):
            hit = jnp.where(shifted == bases[j], -2.0, 0.0)
            w_ref[pl.ds(k * ROWS, ROWS), pl.ds(j * 128, 128)] = hit.astype(BF16)
    links.all_arrived("col", col_rx.at[pl.ds(1, 7)])
    total = col_tx[...]
    for i in range(1, 8):
        total = total + col_rx[i]
    col_inverse = 1.0 / total
    col_tot[pl.ds(0, 8), :] = col_inverse
    links.all_arrived("row", row_rx.at[pl.ds(1, 15)])
    total = row_tx[...]
    for i in range(1, 16):
        total = total + row_rx[i]
    row_tot[pl.ds(0, 16), :] = 1.0 / total
    for place, t in blocks:
        row_tot[pl.ds(16 + q_row(place, t) // ROWS, 1), :] = row_tot[pl.ds(q_index(*place, t), 1), :]
    for k, place in enumerate(ORDER):
        col_tot[pl.ds(8 + k, 1), :] = col_tot[pl.ds(p_index(*place), 1), :]

    def row_factor(k):
        rows = pl.ds(k * ROWS, ROWS)
        factor = jnp.broadcast_to(row_tot[pl.ds(16 + k, 1), :], (128, 128))
        row_inverse[rows, :] = jnp.transpose(factor)

    def weight(k, columns):
        rows = pl.ds(k * ROWS, ROWS)
        factor = row_inverse[rows, :]
        for j in columns:
            cols = pl.ds(j * 128, 128)
            w = e_ref[rows, cols] * (factor + col_tot[pl.ds(8 + j, 1), :])
            w_ref[rows, cols] += w.astype(BF16)

    def weights(slots, columns):
        return [(weight, k, columns) for k in slots]

    def run(work):
        for f, *args in work:
            f(*args)

    def q_dot(first, last, beside=()):
        rows = pl.ds(first, last - first)
        for i in range(4):
            cols = pl.ds(i * 256, 256)
            qpart[rows, cols] = jnp.dot(
                w_ref[rows, :], pbuf[:, cols], preferred_element_type=F32
            ).astype(BF16)
            run(beside[len(beside) * i // 4 : len(beside) * (i + 1) // 4])

    def to_sibling(first, rows, place_row):
        send(
            f"d{place_row}",
            qpart.at[pl.ds(first, rows), :],
            q_d2d.at[pl.ds(place_row, rows), :],
            sibling,
            "d",
        )

    def p_dot(first, last, beside=()):
        out = pl.ds(first, last - first)
        for i in range(4):
            cols = pl.ds(i * 256, 256)
            ppart[out, cols] = lax.dot_general(
                w_ref[:, out],
                qbuf[:, cols],
                (((0,), (0,)), ((), ())),
                preferred_element_type=F32,
            ).astype(BF16)
            run(beside[len(beside) * i // 4 : len(beside) * (i + 1) // 4])

    class Reduce:
        def __init__(self, tag, part, row, extra, rx, right, left, pair):
            self.tag, self.part, self.row, self.extra, self.rx = tag, part, row, extra, rx
            self.to = {"x": right, "l": left, "y": pair}
            self.slots = {}

        def rows(self, place, half):
            return pl.ds(self.row(place) + half * HALF, HALF)

        def total(self, place, half, names):
            value = self.part[self.rows(place, half), :].astype(F32)
            if self.extra is not None:
                rows = pl.ds(PLACE[place] * ROWS + half * HALF, HALF)
                value += self.extra[rows, :].astype(F32)
            for name in names:
                arrived(self.tag + name)
                value += self.rx[self.slots[name]].astype(F32)
            return value

        def send(self, name, place, half, *names):
            if names or self.extra is not None:
                self.part[self.rows(place, half), :] = self.total(place, half, names).astype(BF16)
            self.slots[name] = slot = len(self.slots)
            src = self.part.at[self.rows(place, half), :]
            send(self.tag + name, src, self.rx.at[slot], self.to[name[0]], self.tag)

        def one(self):
            self.send("xB0o", (2, 0), B)
            self.send("lB1o", (2, 1), B)
            self.send("yA2", (2, 1), A)

        def two(self):
            self.send("xB1r", (1, 1), B)
            self.send("yA1", (1, 1), A)
            self.send("yA3", (3, 1), A)

        def three(self):
            self.send("lB1l", (3, 1), B, "lB1o")
            self.send("xAo", (2, 0), A, "yA2")

        def four(self):
            self.send("lB0l", (3, 0), B)
            self.send("xB0r", (1, 0), B, "xB0o")
            self.send("yA0", (0, 1), A)

        def five(self):
            self.send("yB1f", (0, 1), B, "xB1r", "lB1l")

        def six(self):
            self.send("lAl", (3, 0), A, "yA3")
            self.send("xAr", (1, 0), A, "yA1", "xAo")

        def finish(self, unit_ref, length_ref, out_ref):
            for half, names in ((B, ("xB0r", "lB0l", "yB1f")), (A, ("yA0", "lAl", "xAr"))):
                rows = pl.ds(half * HALF, HALF)
                raw = self.total((0, 0), half, names) * SCALE
                unit = unit_ref[rows, :]
                along = jnp.sum(unit * raw, axis=1, keepdims=True)
                out_ref[rows, :] = (raw - unit * along) / length_ref[rows, 0:1]

    qr = Reduce(
        "Q", qpart, lambda place: q_row(place, 0), q_d2d, q_rx,
        q_device(1, 0, 0), q_device(3, 0, 0), q_device(0, 1, 0),
    )
    pr = Reduce(
        "P", ppart, lambda place: PLACE[place] * ROWS, None, p_rx,
        p_device(1, 0), p_device(3, 0), p_device(0, 1),
    )

    for k in range(12, 16):
        row_factor(k)
    run(weights(range(12, 16), range(8)))
    later = [(row_factor, k) for k in range(12)] + weights(range(12), (6, 7))
    q_dot(1792, 2048, later)
    to_sibling(1792, 256, 768)
    p_dot(768, 1024, weights(range(12), (4, 5)))
    pr.one()
    q_dot(1536, 1792, weights(range(8, 12), range(4)))
    arrived("d768")
    qr.one()
    later = weights(range(8), range(4))
    q_dot(1280, 1536, later[:2])
    to_sibling(1280, 256, 512)
    p_dot(512, 768, later[2:6])
    pr.two()
    q_dot(1024, 1280, later[6:])
    arrived("d512")
    qr.two()
    p_dot(128, 512)
    pr.three()
    pr.four()
    qr.three()
    q_dot(640, 1024)
    to_sibling(640, 384, 128)
    q_dot(128, 512)
    q_dot(512, 640)
    to_sibling(512, 128, 0)
    q_dot(0, 128)
    arrived("d128")
    qr.four()
    pr.five()
    p_dot(0, 128)
    pr.six()
    qr.five()
    qr.six()
    arrived("d0")
    pr.finish(pf, p_len, p_out)
    qr.finish(qf, q_len, q_out)
    for sent, like in (
        ("q", q_rx), ("p", p_rx), ("Q", q_rx), ("P", p_rx),
        ("c", q_d2d), ("d", q_d2d),
        ("pos", pos_buf.at[pl.ds(1, 15)]),
        ("row", row_rx.at[pl.ds(1, 15)]),
        ("col", col_rx.at[pl.ds(1, 7)]),
    ):
        links.all_sent(sent, like)


def put_out(q_in, p_in, q_hbm, p_hbm, sem):
    copies = [
        pltpu.make_async_copy(q_in, q_hbm, sem.at[0]),
        pltpu.make_async_copy(p_in, p_hbm, sem.at[1]),
    ]
    for copy in copies:
        copy.start()
    for copy in copies:
        copy.wait()


def per_device(queries, passages, positive):
    vmem = pltpu.VMEM
    scratch = [
        vmem((ROWS, D), F32),
        vmem((ROWS, D), F32),
        vmem((1, ROWS), jnp.int32),
        vmem((ROWS, 128), F32),
        vmem((ROWS, 128), F32),
        vmem((NQ, D), BF16),
        vmem((NP, D), BF16),
        vmem((16, 8, 128), jnp.int32),
        vmem((NQ, NP), F32),
        vmem((NQ, NP), BF16),
        vmem((NQ, 128), F32),
        vmem((8, NP), F32),
        vmem((16, 128), F32),
        vmem((16, 16, 128), F32),
        vmem((8, 128), F32),
        vmem((8, 8, 128), F32),
        vmem((32, 128), F32),
        vmem((16, 128), F32),
        vmem((NQ, D), BF16),
        vmem((NP, D), BF16),
        vmem((1024, D), BF16),
        vmem((14, HALF, D), BF16),
        vmem((14, HALF, D), BF16),
        vmem((NQ, 128), F32),
        pltpu.SemaphoreType.DMA((3,)),
        pltpu.SemaphoreType.DMA((SEMAPHORES,)),
    ]
    out = jax.ShapeDtypeStruct((ROWS, D), F32)
    here = pl.BlockSpec(memory_space=pltpu.VMEM)
    hbm = pl.BlockSpec(memory_space=pltpu.HBM)
    grads = pl.pallas_call(
        kernel,
        out_shape=(out, out),
        in_specs=[hbm, hbm, hbm],
        out_specs=(here, here),
        scratch_shapes=scratch,
        compiler_params=pltpu.CompilerParams(
            collective_id=0, has_side_effects=True, vmem_limit_bytes=52 << 20
        ),
    )(
        pltpu.with_memory_space_constraint(queries, pltpu.HBM),
        pltpu.with_memory_space_constraint(passages, pltpu.HBM),
        pltpu.with_memory_space_constraint(positive.reshape(1, ROWS), pltpu.HBM),
    )
    return pl.pallas_call(
        put_out,
        out_shape=(out, out),
        in_specs=[here, here],
        out_specs=(hbm, hbm),
        scratch_shapes=[pltpu.SemaphoreType.DMA((2,))],
        compiler_params=pltpu.CompilerParams(vmem_limit_bytes=1 << 20),
    )(*grads)


def solution(mesh):
    rows = P(("team", "inner"), None)
    return jax.shard_map(
        per_device,
        mesh=mesh,
        in_specs=(rows, rows, P(("team", "inner"))),
        out_specs=(rows, rows),
        check_vma=False,
    )
```

```python
import math

import jax
import jax.numpy as jnp
from jax import lax
from jax.experimental import pallas as pl
from jax.experimental.pallas import tpu as pltpu
from jax.sharding import PartitionSpec as P

MESH = pl.DeviceIdType.MESH
F32 = jnp.float32
BF16 = jnp.bfloat16

SCALE = 20.0
EXP2_SCALE = SCALE * math.log2(math.e)
EPSILON = 1e-06
RING = 4
ROWS = 128
HALF = 64
D = 1024
NQ = 2048
NP = 1024

PLACE = {
    (0, 0): 0, (0, 1): 1, (3, 0): 2, (1, 0): 3,
    (3, 1): 4, (1, 1): 5, (2, 0): 6, (2, 1): 7,
}
ORDER = sorted(PLACE, key=PLACE.get)
A, B = 0, 1
SEMAPHORES = 75


def q_row(place, t):
    k = PLACE[place]
    return t * 512 + k * ROWS if k < 4 else k // 2 * 512 + t * 256 + k % 2 * ROWS


class Links:
    def __init__(self, semaphores, device):
        self.semaphores, self.device = semaphores, device
        self.index, self.copies = {}, {}

    def semaphore(self, name):
        i = self.index.setdefault(name, len(self.index))
        assert i < SEMAPHORES
        return self.semaphores.at[i]

    def copy(self, src, dst, sent, landed, device):
        return pltpu.make_async_remote_copy(
            src_ref=src,
            dst_ref=dst,
            send_sem=self.semaphore("sent " + sent),
            recv_sem=self.semaphore("landed " + landed),
            device_id=device,
            device_id_type=MESH,
        )

    def send(self, name, src, dst, device, sent, landed=None):
        copy = self.copy(src, dst, sent, landed or name, device)
        copy.start()
        assert name not in self.copies
        self.copies[name] = copy

    def arrived(self, name):
        self.copies[name].wait_recv()

    def all_arrived(self, landed, like):
        self.copy(like, like, "c", landed, self.device).wait_recv()

    def all_sent(self, sent, like):
        self.copy(like, like, sent, "c1", self.device).wait_send()


def kernel(
    q_hbm, p_hbm, pos_hbm, q_out, p_out,
    qf, pf, pos_in, q_inverse, p_inverse, qbuf, pbuf, pos_buf, e_ref, w_ref, racc, cacc,
    row_tx, row_rx, col_tx, col_rx, row_tot, col_tot, qpart, ppart, q_d2d, q_rx, p_rx,
    row_inverse, local_sem, copy_sem,
):
    team, inner = lax.axis_index("team"), lax.axis_index("inner")
    x, c = team // 2, team % 2
    z, y = inner // RING, inner % RING
    bit = y % 2

    def device(x, y, z, c):
        return {"team": x * 2 + c, "inner": z * RING + y}

    def q_device(r, s, t):
        yy = y if s == 0 else y + 1 - 2 * bit
        return device((x + r) % RING, yy, z, c if t == 0 else 1 - c)

    def p_device(r, s):
        return device(x, y if s == 0 else 3 - y, (z + r) % RING, c)

    q_peers = [(r, s, t) for r in range(RING) for s in range(2) for t in range(2)][1:]
    p_peers = [(r, s) for r in range(RING) for s in range(2)][1:]

    def far(peer):
        return -min(peer[0], RING - peer[0]) - sum(peer[1:])


    loads = [
        pltpu.make_async_copy(q_hbm, qf, local_sem.at[0]),
        pltpu.make_async_copy(p_hbm, pf, local_sem.at[1]),
        pltpu.make_async_copy(pos_hbm, pos_in, local_sem.at[2]),
    ]
    for load in loads:
        load.start()
    barrier = pltpu.get_barrier_semaphore()
    neighbours = [q_device(*peer) for peer in ((1, 0, 0), (3, 0, 0), (0, 1, 0), (0, 0, 1))]
    neighbours += [p_device(*peer) for peer in ((1, 0), (3, 0), (0, 1))]
    for neighbour in neighbours:
        pl.semaphore_signal(barrier, inc=1, device_id=neighbour, device_id_type=MESH)

    sibling = q_device(0, 0, 1)
    links = Links(copy_sem, sibling)
    send, arrived = links.send, links.arrived

    def normalize(full, inverse_ref, rounded):
        v = full[...]
        inverse = 1.0 / jnp.sqrt(jnp.sum(v * v, axis=1, keepdims=True) + EPSILON)
        unit = v * inverse
        full[...] = unit
        inverse_ref[...] = jnp.broadcast_to(inverse, (ROWS, 128))
        rounded[pl.ds(0, ROWS), :] = unit.astype(BF16)

    loads[0].wait()
    normalize(qf, q_inverse, qbuf)
    loads[1].wait()
    normalize(pf, p_inverse, pbuf)
    pl.semaphore_wait(barrier, len(neighbours))

    def q_at(place, half, t=0):
        return qbuf.at[pl.ds(q_row(place, t) + half * HALF, HALF), :]

    def p_at(place, half):
        return pbuf.at[pl.ds(PLACE[place] * ROWS + half * HALF, HALF), :]

    class Gather:
        def __init__(self, tag, at, right, left, pair, on_arrival):
            self.tag, self.at, self.on_arrival = tag, at, on_arrival
            self.to = {"x": right, "l": left, "y": pair}
            self.landed = {}

        def send(self, name, src, dst, half):
            self.landed[name] = (dst, half)
            send(self.tag + name, self.at(src, half), self.at(dst, half), self.to[name[0]], self.tag)

        def take(self, name):
            arrived(self.tag + name)
            self.on_arrival(name, *self.landed[name])

        def begin(self):
            self.send("xA", (0, 0), (3, 0), A)
            self.send("lA", (0, 0), (1, 0), A)
            self.send("yB", (0, 0), (0, 1), B)
            self.send("xB", (0, 0), (3, 0), B)
            self.send("lB", (0, 0), (1, 0), B)
            self.send("yA", (0, 0), (0, 1), A)

        def first(self):
            self.take("xA")
            self.send("xA2", (3, 0), (2, 0), A)
            self.send("yA3", (3, 0), (3, 1), A)
            self.take("lA")
            self.send("yA1", (1, 0), (1, 1), A)
            self.take("yB")
            self.send("xPB", (0, 1), (3, 1), B)
            self.send("lPB", (0, 1), (1, 1), B)

        def second(self):
            self.take("xB")
            self.send("xB2", (3, 0), (2, 0), B)
            self.take("lB")
            self.take("yA")

        def third(self):
            self.take("lPB")
            self.send("lPB2", (1, 1), (2, 1), B)
            self.take("xA2")
            self.send("yA2", (2, 0), (2, 1), A)
            self.take("yA3")

        def fourth(self):
            self.take("xPB")
            self.take("yA1")

        def fifth(self):
            self.take("xB2")
            self.take("yA2")

    def share(name, place, half):
        stage = "c1" if PLACE[place] < 4 else "c2" if PLACE[place] < 6 else "c3"
        send("c" + name, q_at(place, half, 0), q_at(place, half, 1), sibling, "c", stage)

    qg = Gather("q", q_at, q_device(1, 0, 0), q_device(3, 0, 0), q_device(0, 1, 0), share)
    pg = Gather("p", p_at, p_device(1, 0), p_device(3, 0), p_device(0, 1), lambda *_: None)
    qg.begin()
    pg.begin()
    send("c", qbuf.at[pl.ds(0, ROWS), :], qbuf.at[pl.ds(512, ROWS), :], sibling, "c", "c1")
    loads[2].wait()
    pos_buf[0] = jnp.broadcast_to(pos_in[...], (8, 128))
    racc[...] = jnp.zeros_like(racc)
    cacc[...] = jnp.zeros_like(cacc)

    def scores(rows0, rows1, cols0, cols1):
        step = width = 256
        for i in range(rows0, rows1, step):
            rows = pl.ds(i, step)
            for j in range(cols0, cols1, width):
                cols = pl.ds(j, width)
                s = lax.dot_general(
                    qbuf[rows, :],
                    pbuf[cols, :],
                    (((1,), (1,)), ((), ())),
                    preferred_element_type=F32,
                )
                e = jnp.exp2(s * EXP2_SCALE)
                e_ref[rows, cols] = e
                part = e[:, 0:128]
                for k in range(128, width, 128):
                    part = part + e[:, k : k + 128]
                racc[rows, :] += part
                cacc[:, cols] += jnp.sum(e.reshape(step // 8, 8, width), axis=0)

    def q_index(r, s, t):
        yb = bit if s == 0 else 1 - bit
        return ((x + r) % RING) * 4 + yb * 2 + (c if t == 0 else 1 - c)

    def sum_rows(blocks):
        for place, t in blocks:
            turned = jnp.transpose(racc[pl.ds(q_row(place, t), ROWS), :])
            row_tx[pl.ds(q_index(*place, t), 1), :] = jnp.sum(turned, axis=0, keepdims=True)

    def landed(stage, rows, count):
        links.all_arrived(stage, qbuf.at[pl.ds(rows, count), :])

    for g in (qg, pg):
        g.first()
    for g in (qg, pg):
        g.second()
    scores(0, 512, 0, 512)
    landed("c1", 512, 512)
    for g in (qg, pg):
        g.third()
    scores(512, 1024, 0, 512)
    for g in (qg, pg):
        g.fourth()
    scores(0, 1024, 512, 768)
    scores(1024, 1280, 0, 768)
    for g in (qg, pg):
        g.take("lPB2")
    landed("c2", 1280, 256)
    scores(1280, 1536, 0, 768)
    for g in (qg, pg):
        g.fifth()
    blocks = sorted(((place, t) for place in ORDER for t in range(2)), key=lambda b: q_row(*b))
    for r, s, t in q_peers:
        slot = q_row((-r % RING, s), t) // ROWS
        send(f"pos{r}{s}{t}", pos_buf.at[0], pos_buf.at[slot], q_device(r, s, t), "pos", "pos")
    scores(0, 1536, 768, 1024)
    scores(1536, 1792, 0, 1024)
    sum_rows(blocks[:-2])
    landed("c3", 1792, 256)
    scores(1792, 2048, 0, 1024)

    def p_index(r, s):
        yb = bit if s == 0 else 1 - bit
        return ((z + r) % RING) * 2 + yb

    for k, place in enumerate(ORDER):
        col = jnp.sum(cacc[:, pl.ds(k * ROWS, ROWS)], axis=0, keepdims=True)
        col_tx[pl.ds(p_index(*place), 1), :] = col
    for r, s in sorted(p_peers, key=far):
        slot = (-r % RING) * 2 + s
        send(f"col{r}{s}", col_tx, col_rx.at[slot], p_device(r, s), "col", "col")
    sum_rows(blocks[-2:])
    for r, s, t in sorted(q_peers, key=far):
        slot = (-r % RING) * 4 + s * 2 + t
        send(f"row{r}{s}{t}", row_tx, row_rx.at[slot], q_device(r, s, t), "row", "row")

    def column_base(place):
        r, s = place
        zz, yy = (z + r) % RING, y if s == 0 else 3 - y
        return (team * 16 + zz * RING + yy) * ROWS

    bases = [column_base(place).astype(F32) for place in ORDER]

    links.all_arrived("pos", pos_buf.at[pl.ds(1, 15)])
    lane = lax.broadcasted_iota(jnp.int32, (ROWS, 128), 1).astype(F32)
    for k in range(16):
        target = jnp.broadcast_to(pos_buf[k, pl.ds(0, 1), :].astype(F32), (128, 128))
        shifted = jnp.transpose(target) - lane
        for j in range(8):
            hit = jnp.where(shifted == bases[j], -2.0, 0.0)
            w_ref[pl.ds(k * ROWS, ROWS), pl.ds(j * 128, 128)] = hit.astype(BF16)
    links.all_arrived("col", col_rx.at[pl.ds(1, 7)])
    total = col_tx[...]
    for i in range(1, 8):
        total = total + col_rx[i]
    col_inverse = 1.0 / total
    col_tot[pl.ds(0, 8), :] = col_inverse
    links.all_arrived("row", row_rx.at[pl.ds(1, 15)])
    total = row_tx[...]
    for i in range(1, 16):
        total = total + row_rx[i]
    row_tot[pl.ds(0, 16), :] = 1.0 / total
    for place, t in blocks:
        row_tot[pl.ds(16 + q_row(place, t) // ROWS, 1), :] = row_tot[pl.ds(q_index(*place, t), 1), :]
    for k, place in enumerate(ORDER):
        col_tot[pl.ds(8 + k, 1), :] = col_tot[pl.ds(p_index(*place), 1), :]

    def row_factor(k):
        rows = pl.ds(k * ROWS, ROWS)
        factor = jnp.broadcast_to(row_tot[pl.ds(16 + k, 1), :], (128, 128))
        row_inverse[rows, :] = jnp.transpose(factor)

    def weight(k, columns):
        rows = pl.ds(k * ROWS, ROWS)
        factor = row_inverse[rows, :]
        for j in columns:
            cols = pl.ds(j * 128, 128)
            w = e_ref[rows, cols] * (factor + col_tot[pl.ds(8 + j, 1), :])
            w_ref[rows, cols] += w.astype(BF16)

    def weights(slots, columns):
        return [(weight, k, columns) for k in slots]

    def run(work):
        for f, *args in work:
            f(*args)

    def q_dot(first, last, beside=()):
        rows = pl.ds(first, last - first)
        for i in range(4):
            cols = pl.ds(i * 256, 256)
            qpart[rows, cols] = jnp.dot(
                w_ref[rows, :], pbuf[:, cols], preferred_element_type=F32
            ).astype(BF16)
            run(beside[len(beside) * i // 4 : len(beside) * (i + 1) // 4])

    def to_sibling(first, rows, place_row):
        send(
            f"d{place_row}",
            qpart.at[pl.ds(first, rows), :],
            q_d2d.at[pl.ds(place_row, rows), :],
            sibling,
            "d",
        )

    def p_dot(first, last, beside=()):
        out = pl.ds(first, last - first)
        for i in range(4):
            cols = pl.ds(i * 256, 256)
            ppart[out, cols] = lax.dot_general(
                w_ref[:, out],
                qbuf[:, cols],
                (((0,), (0,)), ((), ())),
                preferred_element_type=F32,
            ).astype(BF16)
            run(beside[len(beside) * i // 4 : len(beside) * (i + 1) // 4])

    class Reduce:
        def __init__(self, tag, part, row, extra, rx, right, left, pair):
            self.tag, self.part, self.row, self.extra, self.rx = tag, part, row, extra, rx
            self.to = {"x": right, "l": left, "y": pair}
            self.slots = {}

        def rows(self, place, half):
            return pl.ds(self.row(place) + half * HALF, HALF)

        def total(self, place, half, names):
            value = self.part[self.rows(place, half), :].astype(F32)
            if self.extra is not None:
                rows = pl.ds(PLACE[place] * ROWS + half * HALF, HALF)
                value += self.extra[rows, :].astype(F32)
            for name in names:
                arrived(self.tag + name)
                value += self.rx[self.slots[name]].astype(F32)
            return value

        def send(self, name, place, half, *names):
            if names or self.extra is not None:
                self.part[self.rows(place, half), :] = self.total(place, half, names).astype(BF16)
            self.slots[name] = slot = len(self.slots)
            src = self.part.at[self.rows(place, half), :]
            send(self.tag + name, src, self.rx.at[slot], self.to[name[0]], self.tag)

        def one(self):
            self.send("xB0o", (2, 0), B)
            self.send("lB1o", (2, 1), B)
            self.send("yA2", (2, 1), A)

        def two(self):
            self.send("xB1r", (1, 1), B)
            self.send("yA1", (1, 1), A)
            self.send("yA3", (3, 1), A)

        def three(self):
            self.send("lB1l", (3, 1), B, "lB1o")
            self.send("xAo", (2, 0), A, "yA2")

        def four(self):
            self.send("lB0l", (3, 0), B)
            self.send("xB0r", (1, 0), B, "xB0o")
            self.send("yA0", (0, 1), A)

        def five(self):
            self.send("yB1f", (0, 1), B, "xB1r", "lB1l")

        def six(self):
            self.send("lAl", (3, 0), A, "yA3")
            self.send("xAr", (1, 0), A, "yA1", "xAo")

        def finish(self, unit_ref, inverse_ref, out_ref):
            for half, names in ((B, ("xB0r", "lB0l", "yB1f")), (A, ("yA0", "lAl", "xAr"))):
                rows = pl.ds(half * HALF, HALF)
                raw = self.total((0, 0), half, names) * SCALE
                unit = unit_ref[rows, :]
                along = jnp.sum(unit * raw, axis=1, keepdims=True)
                out_ref[rows, :] = (raw - unit * along) * inverse_ref[rows, 0:1]

    qr = Reduce(
        "Q", qpart, lambda place: q_row(place, 0), q_d2d, q_rx,
        q_device(1, 0, 0), q_device(3, 0, 0), q_device(0, 1, 0),
    )
    pr = Reduce(
        "P", ppart, lambda place: PLACE[place] * ROWS, None, p_rx,
        p_device(1, 0), p_device(3, 0), p_device(0, 1),
    )

    for k in range(12, 16):
        row_factor(k)
    run(weights(range(12, 16), range(8)))
    later = [(row_factor, k) for k in range(12)] + weights(range(12), (6, 7))
    q_dot(1792, 2048, later)
    to_sibling(1792, 256, 768)
    p_dot(768, 1024, weights(range(12), (4, 5)))
    pr.one()
    q_dot(1536, 1792, weights(range(8, 12), range(4)))
    arrived("d768")
    qr.one()
    later = weights(range(8), range(4))
    q_dot(1280, 1536, later[:2])
    to_sibling(1280, 256, 512)
    p_dot(512, 768, later[2:6])
    pr.two()
    q_dot(1024, 1280, later[6:])
    arrived("d512")
    qr.two()
    p_dot(128, 512)
    pr.three()
    pr.four()
    qr.three()
    q_dot(640, 1024)
    to_sibling(640, 384, 128)
    q_dot(128, 512)
    q_dot(512, 640)
    to_sibling(512, 128, 0)
    q_dot(0, 128)
    arrived("d128")
    qr.four()
    pr.five()
    p_dot(0, 128)
    pr.six()
    qr.five()
    qr.six()
    arrived("d0")
    pr.finish(pf, p_inverse, p_out)
    qr.finish(qf, q_inverse, q_out)
    for sent, like in (
        ("q", q_rx), ("p", p_rx), ("Q", q_rx), ("P", p_rx),
        ("c", q_d2d), ("d", q_d2d),
        ("pos", pos_buf.at[pl.ds(1, 15)]),
        ("row", row_rx.at[pl.ds(1, 15)]),
        ("col", col_rx.at[pl.ds(1, 7)]),
    ):
        links.all_sent(sent, like)


def put_out(q_in, p_in, q_hbm, p_hbm, sem):
    copies = [
        pltpu.make_async_copy(q_in, q_hbm, sem.at[0]),
        pltpu.make_async_copy(p_in, p_hbm, sem.at[1]),
    ]
    for copy in copies:
        copy.start()
    for copy in copies:
        copy.wait()


def per_device(queries, passages, positive):
    vmem = pltpu.VMEM
    scratch = [
        vmem((ROWS, D), F32),
        vmem((ROWS, D), F32),
        vmem((1, ROWS), jnp.int32),
        vmem((ROWS, 128), F32),
        vmem((ROWS, 128), F32),
        vmem((NQ, D), BF16),
        vmem((NP, D), BF16),
        vmem((16, 8, 128), jnp.int32),
        vmem((NQ, NP), F32),
        vmem((NQ, NP), BF16),
        vmem((NQ, 128), F32),
        vmem((8, NP), F32),
        vmem((16, 128), F32),
        vmem((16, 16, 128), F32),
        vmem((8, 128), F32),
        vmem((8, 8, 128), F32),
        vmem((32, 128), F32),
        vmem((16, 128), F32),
        vmem((NQ, D), BF16),
        vmem((NP, D), BF16),
        vmem((1024, D), BF16),
        vmem((14, HALF, D), BF16),
        vmem((14, HALF, D), BF16),
        vmem((NQ, 128), F32),
        pltpu.SemaphoreType.DMA((3,)),
        pltpu.SemaphoreType.DMA((SEMAPHORES,)),
    ]
    out = jax.ShapeDtypeStruct((ROWS, D), F32)
    here = pl.BlockSpec(memory_space=pltpu.VMEM)
    hbm = pl.BlockSpec(memory_space=pltpu.HBM)
    grads = pl.pallas_call(
        kernel,
        out_shape=(out, out),
        in_specs=[hbm, hbm, hbm],
        out_specs=(here, here),
        scratch_shapes=scratch,
        compiler_params=pltpu.CompilerParams(
            collective_id=0, has_side_effects=True, vmem_limit_bytes=52 << 20
        ),
    )(
        pltpu.with_memory_space_constraint(queries, pltpu.HBM),
        pltpu.with_memory_space_constraint(passages, pltpu.HBM),
        pltpu.with_memory_space_constraint(positive.reshape(1, ROWS), pltpu.HBM),
    )
    return pl.pallas_call(
        put_out,
        out_shape=(out, out),
        in_specs=[here, here],
        out_specs=(hbm, hbm),
        scratch_shapes=[pltpu.SemaphoreType.DMA((2,))],
        compiler_params=pltpu.CompilerParams(vmem_limit_bytes=1 << 20),
    )(*grads)


def solution(mesh):
    rows = P(("team", "inner"), None)
    return jax.shard_map(
        per_device,
        mesh=mesh,
        in_specs=(rows, rows, P(("team", "inner"))),
        out_specs=(rows, rows),
        check_vma=False,
    )
```

```python
import math

import jax
import jax.numpy as jnp
from jax import lax
from jax.experimental import pallas as pl
from jax.experimental.pallas import tpu as pltpu
from jax.sharding import PartitionSpec as P

MESH = pl.DeviceIdType.MESH
F32 = jnp.float32
BF16 = jnp.bfloat16

SCALE = 20.0
EXP2_SCALE = SCALE * math.log2(math.e)
EPSILON = 1e-06
RING = 4
ROWS = 128
HALF = 64
D = 1024
NQ = 2048
NP = 1024

PLACE = {
    (0, 0): 0, (0, 1): 1, (3, 0): 2, (1, 0): 3,
    (3, 1): 4, (1, 1): 5, (2, 0): 6, (2, 1): 7,
}
ORDER = sorted(PLACE, key=PLACE.get)
A, B = 0, 1
SEMAPHORES = 75


def q_row(place, t):
    k = PLACE[place]
    return t * 512 + k * ROWS if k < 4 else k // 2 * 512 + t * 256 + k % 2 * ROWS


class Links:
    def __init__(self, semaphores, device):
        self.semaphores, self.device = semaphores, device
        self.index, self.copies = {}, {}

    def semaphore(self, name):
        i = self.index.setdefault(name, len(self.index))
        assert i < SEMAPHORES
        return self.semaphores.at[i]

    def copy(self, src, dst, sent, landed, device):
        return pltpu.make_async_remote_copy(
            src_ref=src,
            dst_ref=dst,
            send_sem=self.semaphore("sent " + sent),
            recv_sem=self.semaphore("landed " + landed),
            device_id=device,
            device_id_type=MESH,
        )

    def send(self, name, src, dst, device, sent, landed=None):
        copy = self.copy(src, dst, sent, landed or name, device)
        copy.start()
        assert name not in self.copies
        self.copies[name] = copy

    def arrived(self, name):
        self.copies[name].wait_recv()

    def all_arrived(self, landed, like):
        self.copy(like, like, "c", landed, self.device).wait_recv()

    def all_sent(self, sent, like):
        self.copy(like, like, sent, "c1", self.device).wait_send()


def kernel(
    q_hbm, p_hbm, pos_hbm, q_out, p_out,
    qf, pf, pos_in, q_inverse, p_inverse, qbuf, pbuf, pos_buf, e_ref, w_ref, racc, cacc,
    row_tx, row_rx, col_tx, col_rx, row_tot, col_tot, qpart, ppart, q_d2d, q_rx, p_rx,
    row_inverse, local_sem, copy_sem,
):
    team, inner = lax.axis_index("team"), lax.axis_index("inner")
    x, c = team // 2, team % 2
    z, y = inner // RING, inner % RING
    bit = y % 2

    def device(x, y, z, c):
        return {"team": x * 2 + c, "inner": z * RING + y}

    def q_device(r, s, t):
        yy = y if s == 0 else y + 1 - 2 * bit
        return device((x + r) % RING, yy, z, c if t == 0 else 1 - c)

    def p_device(r, s):
        return device(x, y if s == 0 else 3 - y, (z + r) % RING, c)

    q_peers = [(r, s, t) for r in range(RING) for s in range(2) for t in range(2)][1:]
    p_peers = [(r, s) for r in range(RING) for s in range(2)][1:]

    def far(peer):
        return -min(peer[0], RING - peer[0]) - sum(peer[1:])


    loads = [
        pltpu.make_async_copy(q_hbm, qf, local_sem.at[0]),
        pltpu.make_async_copy(p_hbm, pf, local_sem.at[1]),
        pltpu.make_async_copy(pos_hbm, pos_in, local_sem.at[2]),
    ]
    for load in loads:
        load.start()
    barrier = pltpu.get_barrier_semaphore()
    neighbours = [q_device(*peer) for peer in ((1, 0, 0), (3, 0, 0), (0, 1, 0), (0, 0, 1))]
    neighbours += [p_device(*peer) for peer in ((1, 0), (3, 0), (0, 1))]
    for neighbour in neighbours:
        pl.semaphore_signal(barrier, inc=1, device_id=neighbour, device_id_type=MESH)

    sibling = q_device(0, 0, 1)
    links = Links(copy_sem, sibling)
    send, arrived = links.send, links.arrived

    def normalize(full, inverse_ref, rounded):
        v = full[...]
        inverse = 1.0 / jnp.sqrt(jnp.sum(v * v, axis=1, keepdims=True) + EPSILON)
        unit = v * inverse
        full[...] = unit
        inverse_ref[...] = jnp.broadcast_to(inverse, (ROWS, 128))
        rounded[pl.ds(0, ROWS), :] = unit.astype(BF16)

    loads[0].wait()
    normalize(qf, q_inverse, qbuf)
    loads[1].wait()
    normalize(pf, p_inverse, pbuf)
    pl.semaphore_wait(barrier, len(neighbours))

    def q_at(place, half, t=0):
        return qbuf.at[pl.ds(q_row(place, t) + half * HALF, HALF), :]

    def p_at(place, half):
        return pbuf.at[pl.ds(PLACE[place] * ROWS + half * HALF, HALF), :]

    class Gather:
        def __init__(self, tag, at, right, left, pair, on_arrival):
            self.tag, self.at, self.on_arrival = tag, at, on_arrival
            self.to = {"x": right, "l": left, "y": pair}
            self.landed = {}

        def send(self, name, src, dst, half):
            self.landed[name] = (dst, half)
            send(self.tag + name, self.at(src, half), self.at(dst, half), self.to[name[0]], self.tag)

        def take(self, name):
            arrived(self.tag + name)
            self.on_arrival(name, *self.landed[name])

        def begin(self):
            self.send("xA", (0, 0), (3, 0), A)
            self.send("lA", (0, 0), (1, 0), A)
            self.send("yB", (0, 0), (0, 1), B)
            self.send("xB", (0, 0), (3, 0), B)
            self.send("lB", (0, 0), (1, 0), B)
            self.send("yA", (0, 0), (0, 1), A)

        def first(self):
            self.take("xA")
            self.send("xA2", (3, 0), (2, 0), A)
            self.send("yA3", (3, 0), (3, 1), A)
            self.take("lA")
            self.send("yA1", (1, 0), (1, 1), A)
            self.take("yB")
            self.send("xPB", (0, 1), (3, 1), B)
            self.send("lPB", (0, 1), (1, 1), B)

        def second(self):
            self.take("xB")
            self.send("xB2", (3, 0), (2, 0), B)
            self.take("lB")
            self.take("yA")

        def third(self):
            self.take("lPB")
            self.send("lPB2", (1, 1), (2, 1), B)
            self.take("xA2")
            self.send("yA2", (2, 0), (2, 1), A)
            self.take("yA3")

        def fourth(self):
            self.take("xPB")
            self.take("yA1")

        def fifth(self):
            self.take("xB2")
            self.take("yA2")

    def share(name, place, half):
        stage = "c1" if PLACE[place] < 4 else "c2" if PLACE[place] < 6 else "c3"
        send("c" + name, q_at(place, half, 0), q_at(place, half, 1), sibling, "c", stage)

    qg = Gather("q", q_at, q_device(1, 0, 0), q_device(3, 0, 0), q_device(0, 1, 0), share)
    pg = Gather("p", p_at, p_device(1, 0), p_device(3, 0), p_device(0, 1), lambda *_: None)
    qg.begin()
    pg.begin()
    send("c", qbuf.at[pl.ds(0, ROWS), :], qbuf.at[pl.ds(512, ROWS), :], sibling, "c", "c1")
    loads[2].wait()
    pos_buf[0] = jnp.broadcast_to(pos_in[...], (8, 128))
    racc[...] = jnp.zeros_like(racc)
    cacc[...] = jnp.zeros_like(cacc)

    def scores(rows0, rows1, cols0, cols1):
        step = width = 256
        for i in range(rows0, rows1, step):
            rows = pl.ds(i, step)
            for j in range(cols0, cols1, width):
                cols = pl.ds(j, width)
                s = lax.dot_general(
                    qbuf[rows, :],
                    pbuf[cols, :],
                    (((1,), (1,)), ((), ())),
                    preferred_element_type=F32,
                )
                e = jnp.exp2(s * EXP2_SCALE)
                e_ref[rows, cols] = e
                part = e[:, 0:128]
                for k in range(128, width, 128):
                    part = part + e[:, k : k + 128]
                racc[rows, :] += part
                cacc[:, cols] += jnp.sum(e.reshape(step // 8, 8, width), axis=0)

    def q_index(r, s, t):
        yb = bit if s == 0 else 1 - bit
        return ((x + r) % RING) * 4 + yb * 2 + (c if t == 0 else 1 - c)

    def sum_rows(blocks):
        for place, t in blocks:
            turned = jnp.transpose(racc[pl.ds(q_row(place, t), ROWS), :])
            row_tx[pl.ds(q_index(*place, t), 1), :] = jnp.sum(turned, axis=0, keepdims=True)

    def landed(stage, rows, count):
        links.all_arrived(stage, qbuf.at[pl.ds(rows, count), :])

    for g in (qg, pg):
        g.first()
    for g in (qg, pg):
        g.second()
    scores(0, 512, 0, 512)
    landed("c1", 512, 512)
    for g in (qg, pg):
        g.third()
    scores(512, 1024, 0, 512)
    for g in (qg, pg):
        g.fourth()
    scores(0, 1024, 512, 768)
    scores(1024, 1280, 0, 768)
    for g in (qg, pg):
        g.take("lPB2")
    landed("c2", 1280, 256)
    scores(1280, 1536, 0, 768)
    for g in (qg, pg):
        g.fifth()
    blocks = sorted(((place, t) for place in ORDER for t in range(2)), key=lambda b: q_row(*b))
    for r, s, t in q_peers:
        slot = q_row((-r % RING, s), t) // ROWS
        send(f"pos{r}{s}{t}", pos_buf.at[0], pos_buf.at[slot], q_device(r, s, t), "pos", "pos")
    scores(0, 1536, 768, 1024)
    scores(1536, 1792, 0, 1024)
    sum_rows(blocks[:-2])
    landed("c3", 1792, 256)
    scores(1792, 2048, 0, 1024)

    def p_index(r, s):
        yb = bit if s == 0 else 1 - bit
        return ((z + r) % RING) * 2 + yb

    for k, place in enumerate(ORDER):
        col = jnp.sum(cacc[:, pl.ds(k * ROWS, ROWS)], axis=0, keepdims=True)
        col_tx[pl.ds(p_index(*place), 1), :] = col
    for r, s in sorted(p_peers, key=far):
        slot = (-r % RING) * 2 + s
        send(f"col{r}{s}", col_tx, col_rx.at[slot], p_device(r, s), "col", "col")
    sum_rows(blocks[-2:])
    for r, s, t in sorted(q_peers, key=far):
        slot = (-r % RING) * 4 + s * 2 + t
        send(f"row{r}{s}{t}", row_tx, row_rx.at[slot], q_device(r, s, t), "row", "row")

    def column_base(place):
        r, s = place
        zz, yy = (z + r) % RING, y if s == 0 else 3 - y
        return (team * 16 + zz * RING + yy) * ROWS

    bases = [column_base(place).astype(F32) for place in ORDER]

    links.all_arrived("pos", pos_buf.at[pl.ds(1, 15)])
    lane = lax.broadcasted_iota(jnp.int32, (ROWS, 128), 1).astype(F32)
    for k in range(16):
        target = jnp.broadcast_to(pos_buf[k, pl.ds(0, 1), :].astype(F32), (128, 128))
        shifted = jnp.transpose(target) - lane
        for j in range(8):
            hit = jnp.where(shifted == bases[j], -2.0, 0.0)
            w_ref[pl.ds(k * ROWS, ROWS), pl.ds(j * 128, 128)] = hit.astype(BF16)
    links.all_arrived("col", col_rx.at[pl.ds(1, 7)])
    total = col_tx[...]
    for i in range(1, 8):
        total = total + col_rx[i]
    col_inverse = 1.0 / total
    col_tot[pl.ds(0, 8), :] = col_inverse
    links.all_arrived("row", row_rx.at[pl.ds(1, 15)])
    total = row_tx[...]
    for i in range(1, 16):
        total = total + row_rx[i]
    row_tot[pl.ds(0, 16), :] = 1.0 / total
    for place, t in blocks:
        row_tot[pl.ds(16 + q_row(place, t) // ROWS, 1), :] = row_tot[pl.ds(q_index(*place, t), 1), :]
    for k, place in enumerate(ORDER):
        col_tot[pl.ds(8 + k, 1), :] = col_tot[pl.ds(p_index(*place), 1), :]

    def row_factor(k):
        rows = pl.ds(k * ROWS, ROWS)
        factor = jnp.broadcast_to(row_tot[pl.ds(16 + k, 1), :], (128, 128))
        row_inverse[rows, :] = jnp.transpose(factor)

    def weight(k, columns):
        rows = pl.ds(k * ROWS, ROWS)
        factor = row_inverse[rows, :]
        for j in columns:
            cols = pl.ds(j * 128, 128)
            w = e_ref[rows, cols] * (factor + col_tot[pl.ds(8 + j, 1), :])
            w_ref[rows, cols] += w.astype(BF16)

    def weights(slots, columns):
        return [(weight, k, columns) for k in slots]

    def run(work):
        for f, *args in work:
            f(*args)

    def q_dot(first, last, beside=()):
        rows = pl.ds(first, last - first)
        for i in range(4):
            cols = pl.ds(i * 256, 256)
            qpart[rows, cols] = jnp.dot(
                w_ref[rows, :], pbuf[:, cols], preferred_element_type=F32
            ).astype(BF16)
            run(beside[len(beside) * i // 4 : len(beside) * (i + 1) // 4])

    def to_sibling(first, rows, place_row):
        send(
            f"d{place_row}",
            qpart.at[pl.ds(first, rows), :],
            q_d2d.at[pl.ds(place_row, rows), :],
            sibling,
            "d",
        )

    def p_dot(first, last, beside=()):
        out = pl.ds(first, last - first)
        for i in range(4):
            cols = pl.ds(i * 256, 256)
            ppart[out, cols] = lax.dot_general(
                w_ref[:, out],
                qbuf[:, cols],
                (((0,), (0,)), ((), ())),
                preferred_element_type=F32,
            ).astype(BF16)
            run(beside[len(beside) * i // 4 : len(beside) * (i + 1) // 4])

    class Reduce:
        def __init__(self, tag, part, row, extra, rx, right, left, pair):
            self.tag, self.part, self.row, self.extra, self.rx = tag, part, row, extra, rx
            self.to = {"x": right, "l": left, "y": pair}
            self.slots = {}

        def rows(self, place, half):
            return pl.ds(self.row(place) + half * HALF, HALF)

        def total(self, place, half, names):
            value = self.part[self.rows(place, half), :].astype(F32)
            if self.extra is not None:
                rows = pl.ds(PLACE[place] * ROWS + half * HALF, HALF)
                value += self.extra[rows, :].astype(F32)
            for name in names:
                arrived(self.tag + name)
                value += self.rx[self.slots[name]].astype(F32)
            return value

        def send(self, name, place, half, *names):
            if names or self.extra is not None:
                self.part[self.rows(place, half), :] = self.total(place, half, names).astype(BF16)
            self.slots[name] = slot = len(self.slots)
            src = self.part.at[self.rows(place, half), :]
            send(self.tag + name, src, self.rx.at[slot], self.to[name[0]], self.tag)

        def one(self):
            self.send("xB0o", (2, 0), B)
            self.send("lB1o", (2, 1), B)
            self.send("yA2", (2, 1), A)

        def two(self):
            self.send("xB1r", (1, 1), B)
            self.send("yA1", (1, 1), A)
            self.send("yA3", (3, 1), A)

        def three(self):
            self.send("lB1l", (3, 1), B, "lB1o")
            self.send("xAo", (2, 0), A, "yA2")

        def four(self):
            self.send("lB0l", (3, 0), B)
            self.send("xB0r", (1, 0), B, "xB0o")
            self.send("yA0", (0, 1), A)

        def five(self):
            self.send("yB1f", (0, 1), B, "xB1r", "lB1l")

        def six(self):
            self.send("lAl", (3, 0), A, "yA3")
            self.send("xAr", (1, 0), A, "yA1", "xAo")

        def finish(self, unit_ref, inverse_ref, out_ref):
            for half, names in ((B, ("xB0r", "lB0l", "yB1f")), (A, ("yA0", "lAl", "xAr"))):
                rows = pl.ds(half * HALF, HALF)
                raw = self.total((0, 0), half, names) * SCALE
                unit = unit_ref[rows, :]
                along = jnp.sum(unit * raw, axis=1, keepdims=True)
                out_ref[rows, :] = (raw - unit * along) * inverse_ref[rows, 0:1]

    qr = Reduce(
        "Q", qpart, lambda place: q_row(place, 0), q_d2d, q_rx,
        q_device(1, 0, 0), q_device(3, 0, 0), q_device(0, 1, 0),
    )
    pr = Reduce(
        "P", ppart, lambda place: PLACE[place] * ROWS, None, p_rx,
        p_device(1, 0), p_device(3, 0), p_device(0, 1),
    )

    for k in range(12, 16):
        row_factor(k)
    run(weights(range(12, 16), range(8)))
    later = [(row_factor, k) for k in range(12)] + weights(range(12), (6, 7))
    q_dot(1792, 2048, later)
    to_sibling(1792, 256, 768)
    p_dot(768, 1024)
    pr.one()
    q_dot(1536, 1792, weights(range(8, 12), range(6)))
    arrived("d768")
    qr.one()
    later = weights(range(8), range(4))
    q_dot(1280, 1536, weights(range(8), (4, 5)))
    to_sibling(1280, 256, 512)
    p_dot(512, 768, later[:4])
    pr.two()
    q_dot(1024, 1280, later[4:])
    arrived("d512")
    qr.two()
    p_dot(128, 512)
    pr.three()
    pr.four()
    qr.three()
    q_dot(640, 1024)
    to_sibling(640, 384, 128)
    q_dot(128, 512)
    q_dot(512, 640)
    to_sibling(512, 128, 0)
    q_dot(0, 128)
    arrived("d128")
    qr.four()
    pr.five()
    p_dot(0, 128)
    pr.six()
    qr.five()
    qr.six()
    arrived("d0")
    pr.finish(pf, p_inverse, p_out)
    qr.finish(qf, q_inverse, q_out)
    for sent, like in (
        ("q", q_rx), ("p", p_rx), ("Q", q_rx), ("P", p_rx),
        ("c", q_d2d), ("d", q_d2d),
        ("pos", pos_buf.at[pl.ds(1, 15)]),
        ("row", row_rx.at[pl.ds(1, 15)]),
        ("col", col_rx.at[pl.ds(1, 7)]),
    ):
        links.all_sent(sent, like)


def put_out(q_in, p_in, q_hbm, p_hbm, sem):
    copies = [
        pltpu.make_async_copy(q_in, q_hbm, sem.at[0]),
        pltpu.make_async_copy(p_in, p_hbm, sem.at[1]),
    ]
    for copy in copies:
        copy.start()
    for copy in copies:
        copy.wait()


def per_device(queries, passages, positive):
    vmem = pltpu.VMEM
    scratch = [
        vmem((ROWS, D), F32),
        vmem((ROWS, D), F32),
        vmem((1, ROWS), jnp.int32),
        vmem((ROWS, 128), F32),
        vmem((ROWS, 128), F32),
        vmem((NQ, D), BF16),
        vmem((NP, D), BF16),
        vmem((16, 8, 128), jnp.int32),
        vmem((NQ, NP), F32),
        vmem((NQ, NP), BF16),
        vmem((NQ, 128), F32),
        vmem((8, NP), F32),
        vmem((16, 128), F32),
        vmem((16, 16, 128), F32),
        vmem((8, 128), F32),
        vmem((8, 8, 128), F32),
        vmem((32, 128), F32),
        vmem((16, 128), F32),
        vmem((NQ, D), BF16),
        vmem((NP, D), BF16),
        vmem((1024, D), BF16),
        vmem((14, HALF, D), BF16),
        vmem((14, HALF, D), BF16),
        vmem((NQ, 128), F32),
        pltpu.SemaphoreType.DMA((3,)),
        pltpu.SemaphoreType.DMA((SEMAPHORES,)),
    ]
    out = jax.ShapeDtypeStruct((ROWS, D), F32)
    here = pl.BlockSpec(memory_space=pltpu.VMEM)
    hbm = pl.BlockSpec(memory_space=pltpu.HBM)
    grads = pl.pallas_call(
        kernel,
        out_shape=(out, out),
        in_specs=[hbm, hbm, hbm],
        out_specs=(here, here),
        scratch_shapes=scratch,
        compiler_params=pltpu.CompilerParams(
            collective_id=0, has_side_effects=True, vmem_limit_bytes=52 << 20
        ),
    )(
        pltpu.with_memory_space_constraint(queries, pltpu.HBM),
        pltpu.with_memory_space_constraint(passages, pltpu.HBM),
        pltpu.with_memory_space_constraint(positive.reshape(1, ROWS), pltpu.HBM),
    )
    return pl.pallas_call(
        put_out,
        out_shape=(out, out),
        in_specs=[here, here],
        out_specs=(hbm, hbm),
        scratch_shapes=[pltpu.SemaphoreType.DMA((2,))],
        compiler_params=pltpu.CompilerParams(vmem_limit_bytes=1 << 20),
    )(*grads)


def solution(mesh):
    rows = P(("team", "inner"), None)
    return jax.shard_map(
        per_device,
        mesh=mesh,
        in_specs=(rows, rows, P(("team", "inner"))),
        out_specs=(rows, rows),
        check_vma=False,
    )
```
